512 devices in a mesh: dp: 8 (over y_hi, core), expert: 64 (over y_lo, x, z).
Axes of the slice: x: 4, y: 8 (y_hi: 4, y_lo: 2; y = y_hi * 2 + y_lo), z: 8, core: 2. Of those that a mesh axis runs over, the one named last changes fastest.
Arguments:
- weights: bfloat16 [16, 3584, 512], P(None, ('dp', 'expert')), may hold values from -0.09375 to 0.09375
- first_moment: float32 [16, 3584, 512], P(None, ('dp', 'expert')), may hold values from -3 to 3
- second_moment: float32 [16, 3584, 512], P(None, ('dp', 'expert')), may hold values from 0.05 to 2
- placement: int32 [64], replicated, may hold values from 0 to 15, as said below
- block_counts: int32 [8, 64], P('dp', 'expert'), may hold values from 1 to 2
- tokens: bfloat16 [8, 64, 256, 3584], P('dp', 'expert'), may hold values from -6 to 6
- hidden_grad: bfloat16 [8, 64, 256, 256], P('dp', 'expert'), may hold values from -1.1953125 to 1.1953125
Outputs:
- new_weights: bfloat16 [64, 3584, 512], P('expert', 'dp')
- new_first: float32 [64, 3584, 512], P('expert', 'dp')
- new_second: float32 [64, 3584, 512], P('expert', 'dp')
The draws below stay inside these ranges and needn't reach their ends.
Inputs may be any that keep to these rules, and one draw needn't show every extreme that they name: `placement`: every expert block 0 to 15 is owned by at least one device. `block_counts`: the rows after a device's live blocks are padding.
All inputs are finite; a program needn't handle non-finite values.
Results may differ from the reference program's by a relative error of at most 0.015.
Values may be sent and summed in bfloat16 or wider, within the bound.
No kernel may reach another device: no remote copies, remote signals or barrier semaphores. Data moves between devices by JAX's collectives and lax.ppermute only.
A program may use at most 64 MiB of HBM per device.

```python
import math
import jax
import jax.numpy as jnp
from jax import lax

D = 3584
FF_UNIT = 256
BLOCK = 128
MAX_BLOCKS = 2
ROWS = 256
UNITS = 16
N_DP = 8
N_EXPERT = 64


def draw_placement(key, part):
    folded = jax.random.fold_in(key, 17)
    key_first, key_second, key_blocks, key_devices = jax.random.split(folded, 4)
    first_draw = jax.random.randint(key_first, (N_EXPERT,), 0, UNITS)
    second_draw = jax.random.randint(key_second, (N_EXPERT,), 0, UNITS)
    skewed = first_draw * second_draw // UNITS
    device_slot = jnp.arange(N_EXPERT)
    chosen = jnp.where(device_slot < UNITS, device_slot, skewed)
    relabel = jax.random.permutation(key_blocks, UNITS)
    chosen = relabel[chosen]
    shuffle = jax.random.permutation(key_devices, N_EXPERT)
    return chosen[shuffle].astype(jnp.int32)


def plant(drawn, own_key, low, largest):
    spot = [jax.random.randint(jax.random.fold_in(own_key, axis), (), 0, length) for axis, length in enumerate(drawn.shape)]
    longest = drawn.shape.index(max(drawn.shape))
    beside = spot[:longest] + [(spot[longest] + 1) % drawn.shape[longest]] + spot[longest + 1:]
    return drawn.at[tuple(spot)].set(low).at[tuple(beside)].set(largest)


def levels(key, shape, cuts, low, largest):
    def one(dim, parts):
        heights = jax.random.uniform(jax.random.fold_in(jax.random.fold_in(key, 6), dim), (parts,), jnp.float32, low / len(cuts), largest / len(cuts))
        return jnp.repeat(jnp.exp(heights), shape[dim] // parts).reshape((-1,) + (1,) * (len(shape) - dim - 1))

    factor_of = one(*cuts[0])
    for cut in cuts[1:]:
        factor_of = factor_of * one(*cut)
    return factor_of


def gaussian(key, dims, scale, most, pieces=(), held_as=jnp.bfloat16):
    values = jax.random.normal(key, dims, jnp.float32) * scale
    if len(pieces) > 0:
        values = levels(key, dims, pieces, -0.22, 0.18) * values
    return jnp.clip(values, min=-most, max=most).astype(held_as)


def setup_inputs(seed: int = 0) -> dict:
    streams_of = jax.random.split(jax.random.key(seed), 8)
    return {
        "weights": gaussian(streams_of[0], (UNITS, D, 2 * FF_UNIT), D ** -0.5, 0.09375, ((1, 512),)),
        "first_moment": gaussian(streams_of[1], (UNITS, D, 2 * FF_UNIT), 0.5, 3.0, ((1, 512),), jnp.float32),
        "second_moment": jnp.clip(jnp.exp(math.log(2.0) - 3.6888794 * jax.random.uniform(streams_of[2], (UNITS, D, 2 * FF_UNIT), jnp.float32) ** levels(streams_of[2], (UNITS, D, 2 * FF_UNIT), ((1, 512),), -0.2, 0.2)), 0.05, 2.0),
        "placement": draw_placement(jax.random.fold_in(streams_of[7], 71), 0),
        "block_counts": plant(jax.random.randint(streams_of[4], (N_DP, N_EXPERT), 1, MAX_BLOCKS + 1), jax.random.fold_in(streams_of[4], 1), 1, MAX_BLOCKS).astype(jnp.int32),
        "tokens": gaussian(streams_of[5], (N_DP, N_EXPERT, ROWS, D), 1.0, 6.0, ((0, 8), (1, 64))),
        "hidden_grad": gaussian(streams_of[6], (N_DP, N_EXPERT, ROWS, FF_UNIT), 0.2, 1.1953125, ((0, 8), (1, 64))),
    }


beta_first = 0.9
beta_second = 0.95
learning_rate = 0.001
weight_decay = 0.1
adam_epsilon = 1e-08
adam_steps = 10.0

def silu_grads(projected, upstream, live_mask):
    half_width = projected.shape[1] // 2
    gate_part = projected[:, :half_width]
    upward = projected[:, half_width:]
    sigmoid_gate = jax.nn.sigmoid(gate_part)
    masked = jnp.where(live_mask, upstream.astype(jnp.float32), 0.0)
    grad_gate = masked * upward * sigmoid_gate * (1.0 + gate_part * (1.0 - sigmoid_gate))
    grad_upward = masked * gate_part * sigmoid_gate
    return jnp.concatenate([grad_gate, grad_upward], axis=1).astype(jnp.bfloat16)

def adam_update(params, first_moment, second_moment, gradient):
    moment_one = beta_first * first_moment + (1.0 - beta_first) * gradient
    moment_two = beta_second * second_moment + (1.0 - beta_second) * gradient * gradient
    correct_one = 1.0 - beta_first ** adam_steps
    correct_two = 1.0 - beta_second ** adam_steps
    params_full = params.astype(jnp.float32)
    step_size = moment_one / correct_one / (jnp.sqrt(moment_two / correct_two) + adam_epsilon) + weight_decay * params_full
    return ((params_full - learning_rate * step_size).astype(jnp.bfloat16), moment_one, moment_two)

def reference(weights, first_moment, second_moment, placement, block_counts, tokens, hidden_grad):
    dev_tokens = tokens.reshape(N_DP * N_EXPERT, ROWS, D)
    dev_grads = hidden_grad.reshape(N_DP * N_EXPERT, ROWS, FF_UNIT)
    dev_counts = block_counts.reshape(N_DP * N_EXPERT)
    dev_blocks = jnp.tile(placement, N_DP)

    def accumulate(summed, device_item):
        inputs, upstream, counted, block_id = device_item
        matrix = lax.dynamic_index_in_dim(weights, block_id, 0, keepdims=False)
        projected = jnp.dot(inputs, matrix, preferred_element_type=jnp.float32)
        live_mask = (jnp.arange(ROWS) < BLOCK * counted)[:, None]
        grad_proj = silu_grads(projected, upstream, live_mask)
        local_grad = jnp.dot(inputs.T, grad_proj, preferred_element_type=jnp.float32).astype(jnp.bfloat16)
        local_grad = lax.optimization_barrier(local_grad).astype(jnp.float32)
        return (summed.at[block_id].add(local_grad), None)
    zero_grads = jnp.zeros((UNITS, D, 2 * FF_UNIT), jnp.float32)
    gradient = lax.scan(accumulate, zero_grads, (dev_tokens, dev_grads, dev_counts, dev_blocks))[0]
    updated, moment_one, moment_two = adam_update(weights, first_moment, second_moment, gradient)
    return (jnp.take(updated, placement, axis=0), jnp.take(moment_one, placement, axis=0), jnp.take(moment_two, placement, axis=0))
```

```python
import jax
import jax.numpy as jnp
from jax import lax
from jax.sharding import PartitionSpec as P

BLOCK = 128


beta_first = 0.9
beta_second = 0.95
learning_rate = 0.001
weight_decay = 0.1
adam_epsilon = 1e-08
adam_steps = 10.0


def silu_grads(projected, upstream, live_mask):
    half_width = projected.shape[1] // 2
    gate_part = projected[:, :half_width]
    upward = projected[:, half_width:]
    sigmoid_gate = jax.nn.sigmoid(gate_part)
    masked = jnp.where(live_mask, upstream.astype(jnp.float32), 0.0)
    grad_gate = masked * upward * sigmoid_gate * (1.0 + gate_part * (1.0 - sigmoid_gate))
    grad_upward = masked * gate_part * sigmoid_gate
    return jnp.concatenate([grad_gate, grad_upward], axis=1).astype(jnp.bfloat16)


def adam_update(params, first_moment, second_moment, gradient):
    moment_one = beta_first * first_moment + (1.0 - beta_first) * gradient
    moment_two = beta_second * second_moment + (1.0 - beta_second) * gradient * gradient
    correct_one = 1.0 - beta_first**adam_steps
    correct_two = 1.0 - beta_second**adam_steps
    params_full = params.astype(jnp.float32)
    step_size = (
        moment_one / correct_one / (jnp.sqrt(moment_two / correct_two) + adam_epsilon)
        + weight_decay * params_full
    )
    return ((params_full - learning_rate * step_size).astype(jnp.bfloat16), moment_one, moment_two)


def on_device(weights, first_moment, second_moment, placement, block_counts, tokens, hidden_grad):
    expert_count = lax.axis_size("expert")
    block_total = weights.shape[0]
    span_rows = weights.shape[1]
    col_total = weights.shape[2]
    inputs = tokens[0, 0]
    row_total = inputs.shape[0]
    narrow = jnp.bfloat16
    live_mask = (jnp.arange(row_total) < BLOCK * block_counts[0, 0])[:, None]
    own_shape = (expert_count * span_rows, col_total)
    pick = (placement[:, None] == jnp.arange(block_total)[None, :]).astype(narrow)
    same = (placement[:, None] == placement[None, :]).astype(narrow)

    def exchange(values):
        return lax.all_to_all(values, "expert", split_axis=0, concat_axis=0, tiled=True)

    def spread(stored):
        return jnp.einsum("ju,urc->jrc", pick, stored, preferred_element_type=jnp.float32).astype(narrow)

    arrived = exchange(spread(weights))
    own_rows = arrived.reshape(own_shape)
    gathered = lax.all_gather(own_rows, "dp", axis=0, tiled=True)
    moments = jnp.concatenate([first_moment, second_moment], axis=1).astype(narrow)
    moments_sent, _ = lax.optimization_barrier((spread(moments), arrived))
    moments_here = exchange(moments_sent)
    gathered, moments_here = lax.optimization_barrier((gathered, moments_here))
    projected = jnp.dot(inputs, gathered, preferred_element_type=jnp.float32)
    grad_proj = silu_grads(projected, hidden_grad[0, 0], live_mask)
    term = lax.dot_general(
        inputs, grad_proj, (((0,), (0,)), ((), ())), preferred_element_type=jnp.float32
    ).astype(narrow)
    summed_data = lax.psum_scatter(term, "dp", scatter_dimension=0, tiled=True)
    at_home = exchange(summed_data.reshape(expert_count, span_rows, col_total))
    block_grad = jnp.einsum("jk,krc->jrc", same, at_home, preferred_element_type=jnp.float32).astype(narrow)
    grad_here = exchange(block_grad)
    updated, moment_one, moment_two = adam_update(
        own_rows,
        moments_here[:, :span_rows].reshape(own_shape).astype(jnp.float32),
        moments_here[:, span_rows:].reshape(own_shape).astype(jnp.float32),
        grad_here.reshape(own_shape).astype(jnp.float32),
    )
    return (updated[None], moment_one[None], moment_two[None])


def solution(mesh):
    in_specs = (
        P(None, ("dp", "expert"), None),
        P(None, ("dp", "expert"), None),
        P(None, ("dp", "expert"), None),
        P(),
        P("dp", "expert"),
        P("dp", "expert", None, None),
        P("dp", "expert", None, None),
    )
    out_specs = (P("expert", "dp", None), P("expert", "dp", None), P("expert", "dp", None))
    return jax.shard_map(
        on_device, mesh=mesh, in_specs=in_specs, out_specs=out_specs, check_vma=False
    )
```

```python
import jax
import jax.numpy as jnp
from jax import lax
from jax.experimental import pallas as pl
from jax.experimental.pallas import tpu as pltpu
from jax.sharding import PartitionSpec as P

BLOCK = 128


beta_first = 0.9
beta_second = 0.95
learning_rate = 0.001
weight_decay = 0.1
adam_epsilon = 1e-08
adam_steps = 10.0


def adam_update(params, first_moment, second_moment, gradient):
    moment_one = beta_first * first_moment + (1.0 - beta_first) * gradient
    moment_two = beta_second * second_moment + (1.0 - beta_second) * gradient * gradient
    correct_one = 1.0 - beta_first**adam_steps
    correct_two = 1.0 - beta_second**adam_steps
    params_full = params.astype(jnp.float32)
    step_size = (
        moment_one / correct_one / (jnp.sqrt(moment_two / correct_two) + adam_epsilon)
        + weight_decay * params_full
    )
    return ((params_full - learning_rate * step_size).astype(jnp.bfloat16), moment_one, moment_two)


def grad_halves(projected, upstream):
    half_width = projected.shape[1] // 2
    gate_part = projected[:, :half_width]
    upward = projected[:, half_width:]
    sigmoid_gate = jax.nn.sigmoid(gate_part)
    masked = upstream.astype(jnp.float32)
    grad_gate = masked * upward * sigmoid_gate * (1.0 + gate_part * (1.0 - sigmoid_gate))
    grad_upward = masked * gate_part * sigmoid_gate
    return grad_gate.astype(jnp.bfloat16), grad_upward.astype(jnp.bfloat16)


def term_rows(turned_ref, grad_ref, start, count):
    rows = turned_ref[pl.ds(pl.multiple_of(start, 16), count), :]
    return jnp.dot(rows, grad_ref[...], preferred_element_type=jnp.float32).astype(jnp.bfloat16)


def project_kernel(
    place, tok_mine, tok_theirs, turned, hid_mine, hid_theirs, *rest
):
    pieces = rest[:8]
    grad_ref, far_mine, far_theirs, joined = rest[8:]
    chip, core = place[0], place[1]
    count = pieces[0].shape[0]

    def start(step, side):
        other = (core + side) % 2
        return (2 * ((chip + step) % 4) + other) * count

    for slot in range(8):
        joined[pl.ds(pl.multiple_of(start(slot // 2, slot % 2), 16), count), :] = pieces[slot][...]
    half = tok_mine.shape[0]
    width = joined.shape[1] // 2
    for tok, hid, low in ((tok_mine, hid_mine, 0), (tok_theirs, hid_theirs, half)):
        projected = jnp.dot(tok[...], joined[...], preferred_element_type=jnp.float32)
        grad_gate, grad_up = grad_halves(projected, hid[...])
        grad_ref[low : low + half, :width] = grad_gate
        grad_ref[low : low + half, width:] = grad_up
    far_mine[...] = term_rows(turned, grad_ref, start(2, 0), count)
    far_theirs[...] = term_rows(turned, grad_ref, start(2, 1), count)


def turn_kernel(tok_mine, tok_theirs, turned):
    half, wide = tok_mine.shape
    for low, tok in ((0, tok_mine), (half, tok_theirs)):
        for begin in range(0, wide, 512):
            turned[begin : begin + 512, low : low + half] = tok[:, begin : begin + 512].T


def term_kernel(place, turned, grad_ref, *outs):
    chip, core = place[0], place[1]
    count = outs[0].shape[0]
    slot = 0
    for step in (1, 3, 0):
        for side in (0, 1):
            other = (core + side) % 2
            begin = (2 * ((chip + step) % 4) + other) * count
            outs[slot][...] = term_rows(turned, grad_ref, begin, count)
            slot += 1


def in_vmem(count):
    return [pl.BlockSpec(memory_space=pltpu.VMEM) for _ in range(count)]


def in_smem():
    return [pl.BlockSpec(memory_space=pltpu.SMEM)]


def on_device(weights, first_moment, second_moment, placement, block_counts, tokens, hidden_grad):
    expert_count = lax.axis_size("expert")
    dp_count = lax.axis_size("dp")
    chip_count = dp_count // 2
    block_total = weights.shape[0]
    span_rows = weights.shape[1]
    col_total = weights.shape[2]
    inputs = tokens[0, 0]
    row_total, wide = inputs.shape
    narrow = jnp.bfloat16
    own_count = expert_count * span_rows
    own_shape = (own_count, col_total)
    quarter = col_total // 4
    position = lax.axis_index("dp")
    chip, core = position // 2, position % 2
    place = jnp.stack([chip, core]).astype(jnp.int32)
    pick = (placement[:, None] == jnp.arange(block_total)[None, :]).astype(narrow)
    same = (placement[:, None] == placement[None, :]).astype(narrow)

    def exchange(values):
        return lax.all_to_all(values, "expert", split_axis=0, concat_axis=0, tiled=True)

    def spread(stored):
        return jnp.einsum("ju,urc->jrc", pick, stored, preferred_element_type=jnp.float32).astype(narrow)

    def shift(value, step):
        pairs = [
            (2 * h + c, 2 * ((h + step) % chip_count) + c) for h in range(chip_count) for c in range(2)
        ]
        return lax.ppermute(value, "dp", pairs)

    def swap(value):
        return lax.ppermute(value, "dp", [(i, i ^ 1) for i in range(dp_count)])

    def halves(value):
        width = value.shape[1] // 2
        even = [value[:, k : k + quarter] for k in range(0, value.shape[1], 2 * quarter)]
        odd = [value[:, k + quarter : k + 2 * quarter] for k in range(0, value.shape[1], 2 * quarter)]
        even = jnp.concatenate(even, axis=1)
        odd = jnp.concatenate(odd, axis=1)
        return jnp.where(core == 0, even, odd), jnp.where(core == 0, odd, even)

    live_mask = (jnp.arange(row_total) < BLOCK * block_counts[0, 0])[:, None]
    masked = jnp.where(live_mask, hidden_grad[0, 0], jnp.zeros((), narrow))
    hid_mine, hid_give = halves(masked)
    tok_theirs = swap(inputs)
    hid_theirs = swap(hid_give)

    arrived = exchange(spread(weights))
    own_rows = arrived.reshape(own_shape)
    mine, give = halves(own_rows)
    theirs = swap(give)
    plus_mine = shift(mine, 1)
    minus_theirs = shift(theirs, -1)
    minus_mine = shift(mine, -1)
    plus_theirs = shift(theirs, 1)
    far_mine = shift(plus_mine, 1)
    far_theirs = shift(minus_theirs, -1)

    moments = jnp.concatenate([first_moment, second_moment], axis=1).astype(narrow)
    moments_sent, _ = lax.optimization_barrier((spread(moments), arrived))
    moments_here = exchange(moments_sent)

    turned = pl.pallas_call(
        turn_kernel,
        in_specs=in_vmem(2),
        out_specs=in_vmem(1)[0],
        out_shape=jax.ShapeDtypeStruct((wide, 2 * row_total), narrow),
        name="turn",
    )(inputs, tok_theirs)
    piece = jax.ShapeDtypeStruct((own_count, 2 * quarter), narrow)
    grad_proj, send_mine, send_theirs = pl.pallas_call(
        project_kernel,
        in_specs=in_smem() + in_vmem(13),
        out_specs=in_vmem(3),
        out_shape=[jax.ShapeDtypeStruct((2 * row_total, 2 * quarter), narrow), piece, piece],
        scratch_shapes=[pltpu.VMEM((wide, 2 * quarter), narrow)],
        name="project",
    )(
        place, inputs, tok_theirs, turned, hid_mine, hid_theirs,
        mine, theirs, minus_mine, minus_theirs, far_mine, far_theirs, plus_mine, plus_theirs,
    )
    got_plus = shift(send_mine, 1)
    got_minus = shift(send_theirs, -1)
    next_mine, next_theirs, last_mine, last_theirs, sum_mine, sum_theirs = pl.pallas_call(
        term_kernel,
        in_specs=in_smem() + in_vmem(2),
        out_specs=in_vmem(6),
        out_shape=[piece] * 6,
        name="terms",
    )(place, turned, grad_proj)

    def add(*values):
        total = values[0].astype(jnp.float32)
        for value in values[1:]:
            total = total + value.astype(jnp.float32)
        return total.astype(narrow)

    next_mine, last_theirs, moments_here = lax.optimization_barrier((next_mine, last_theirs, moments_here))
    early_theirs = shift(next_theirs, 1)
    early_mine = shift(last_mine, -1)
    late_mine = shift(add(next_mine, got_plus), 1)
    late_theirs = shift(add(last_theirs, got_minus), -1)
    total_theirs = add(sum_theirs, early_theirs, late_theirs)
    total_mine = add(sum_mine, early_mine, late_mine)
    total_other = swap(total_theirs)
    even = jnp.where(core == 0, total_mine, total_other)
    odd = jnp.where(core == 0, total_other, total_mine)
    summed = jnp.concatenate(
        [even[:, :quarter], odd[:, :quarter], even[:, quarter:], odd[:, quarter:]], axis=1
    )
    at_home = exchange(summed.reshape(expert_count, span_rows, col_total))
    block_grad = jnp.einsum("jk,krc->jrc", same, at_home, preferred_element_type=jnp.float32).astype(narrow)
    grad_here = exchange(block_grad)
    updated, moment_one, moment_two = adam_update(
        own_rows,
        moments_here[:, :span_rows].reshape(own_shape).astype(jnp.float32),
        moments_here[:, span_rows:].reshape(own_shape).astype(jnp.float32),
        grad_here.reshape(own_shape).astype(jnp.float32),
    )
    return (updated[None], moment_one[None], moment_two[None])


def solution(mesh):
    in_specs = (
        P(None, ("dp", "expert"), None),
        P(None, ("dp", "expert"), None),
        P(None, ("dp", "expert"), None),
        P(),
        P("dp", "expert"),
        P("dp", "expert", None, None),
        P("dp", "expert", None, None),
    )
    out_specs = (P("expert", "dp", None), P("expert", "dp", None), P("expert", "dp", None))
    return jax.shard_map(
        on_device, mesh=mesh, in_specs=in_specs, out_specs=out_specs, check_vma=False
    )
```

```python
import jax
import jax.numpy as jnp
from jax import lax
from jax.experimental import pallas as pl
from jax.experimental.pallas import tpu as pltpu
from jax.sharding import PartitionSpec as P


BLOCK = 128


beta_first = 0.9
beta_second = 0.95
learning_rate = 0.001
weight_decay = 0.1
adam_epsilon = 1e-08
adam_steps = 10.0


def adam_update(params, first_moment, second_moment, gradient):
    moment_one = beta_first * first_moment + (1.0 - beta_first) * gradient
    moment_two = beta_second * second_moment + (1.0 - beta_second) * gradient * gradient
    correct_one = 1.0 - beta_first**adam_steps
    correct_two = 1.0 - beta_second**adam_steps
    params_full = params.astype(jnp.float32)
    step_size = (
        moment_one / correct_one / (jnp.sqrt(moment_two / correct_two) + adam_epsilon)
        + weight_decay * params_full
    )
    return ((params_full - learning_rate * step_size).astype(jnp.bfloat16), moment_one, moment_two)


def grad_halves(projected, upstream):
    half_width = projected.shape[1] // 2
    gate_part = projected[:, :half_width]
    upward = projected[:, half_width:]
    sigmoid_gate = jax.nn.sigmoid(gate_part)
    masked = upstream.astype(jnp.float32)
    grad_gate = masked * upward * sigmoid_gate * (1.0 + gate_part * (1.0 - sigmoid_gate))
    grad_upward = masked * gate_part * sigmoid_gate
    return grad_gate.astype(jnp.bfloat16), grad_upward.astype(jnp.bfloat16)


def term_rows(turned_ref, grad_ref, start, count):
    rows = turned_ref[pl.ds(pl.multiple_of(start, 16), count), :]
    return jnp.dot(rows, grad_ref[...], preferred_element_type=jnp.float32).astype(jnp.bfloat16)


def piece_start(place, step, side, count):
    return pl.multiple_of((2 * ((place[0] + step) % 4) + (place[1] + side) % 2) * count, 16)


def block_start(place, step, count):
    return pl.multiple_of(((place[0] + step) % 4) * 2 * count, 128)


def join(place, block, mine, theirs):
    count = mine.shape[0]
    core = place[1]
    block[pl.ds(pl.multiple_of(core * count, 16), count), :] = mine[...]
    block[pl.ds(pl.multiple_of((1 - core) * count, 16), count), :] = theirs[...]


def partial_kernel(place, tok_mine, tok_theirs, *rest):
    pieces, partial, block = rest[:6], rest[6], rest[7]
    count = pieces[0].shape[0]
    half = tok_mine.shape[0]
    for slot in range(3):
        join(place, block.at[slot], pieces[2 * slot], pieces[2 * slot + 1])
    for low, tok in ((0, tok_mine), (half, tok_theirs)):
        total = None
        for slot, step in enumerate((0, 1, 3)):
            part = jnp.dot(
                tok[:, pl.ds(block_start(place, step, count), 2 * count)],
                block[slot],
                preferred_element_type=jnp.float32,
            )
            total = part if total is None else total + part
        partial[low : low + half, :] = total


def project_kernel(
    place, partial, hid_mine, hid_theirs, piece_mine, piece_theirs, tok_mine, tok_theirs, turned,
    grad_ref, far_mine, last_mine, block, far_tok, far_rows, last_rows, sems,
):
    count = piece_mine.shape[0]
    half = hid_mine.shape[0]
    lanes = pl.ds(block_start(place, 2, count), 2 * count)
    copies = [
        pltpu.make_async_copy(tok_mine.at[:, lanes], far_tok.at[0:half], sems.at[0]),
        pltpu.make_async_copy(tok_theirs.at[:, lanes], far_tok.at[half : 2 * half], sems.at[1]),
        pltpu.make_async_copy(
            turned.at[pl.ds(piece_start(place, 2, 0, count), count)], far_rows, sems.at[2]
        ),
        pltpu.make_async_copy(
            turned.at[pl.ds(piece_start(place, 3, 0, count), count)], last_rows, sems.at[3]
        ),
    ]
    for copy in copies:
        copy.start()
    join(place, block, piece_mine, piece_theirs)
    width = block.shape[1] // 2
    copies[0].wait()
    copies[1].wait()
    for hid, low in ((hid_mine, 0), (hid_theirs, half)):
        projected = partial[low : low + half, :] + jnp.dot(
            far_tok[low : low + half, :], block[...], preferred_element_type=jnp.float32
        )
        grad_gate, grad_up = grad_halves(projected, hid[...])
        grad_ref[low : low + half, :width] = grad_gate
        grad_ref[low : low + half, width:] = grad_up
    copies[2].wait()
    copies[3].wait()
    grads = grad_ref[...]
    far_mine[...] = jnp.dot(far_rows[...], grads, preferred_element_type=jnp.float32).astype(jnp.bfloat16)
    last_mine[...] = jnp.dot(last_rows[...], grads, preferred_element_type=jnp.float32).astype(jnp.bfloat16)


def turn_kernel(tok_mine, tok_theirs, turned):
    half, wide = tok_mine.shape
    for low, tok in ((0, tok_mine), (half, tok_theirs)):
        for begin in range(0, wide, 512):
            turned[begin : begin + 512, low : low + half] = tok[:, begin : begin + 512].T


def term_kernel(place, turned, grad_ref, *outs):
    count = outs[0].shape[0]
    for slot, (step, side) in enumerate(((2, 1), (1, 0), (1, 1), (3, 1), (0, 0), (0, 1))):
        outs[slot][...] = term_rows(turned, grad_ref, piece_start(place, step, side, count), count)


def adam_kernel(place, params, first, second, gradient, updated, moment_one, moment_two):
    lanes = params.shape[1] // 4
    for kind in range(2):
        for side in range(2):
            read = pl.ds((2 * side + kind) * lanes, lanes)
            into = pl.ds(pl.multiple_of((2 * kind + (place[1] + side) % 2) * lanes, 128), lanes)
            new_params, new_one, new_two = adam_update(
                params[:, read],
                first[:, read].astype(jnp.float32),
                second[:, read].astype(jnp.float32),
                gradient[:, read].astype(jnp.float32),
            )
            updated[0, :, into] = new_params
            moment_one[0, :, into] = new_one
            moment_two[0, :, into] = new_two


def in_vmem(count):
    return [pl.BlockSpec(memory_space=pltpu.VMEM) for _ in range(count)]


def in_smem():
    return [pl.BlockSpec(memory_space=pltpu.SMEM)]


def in_any(count):
    return [pl.BlockSpec(memory_space=pl.ANY) for _ in range(count)]


def on_device(weights, first_moment, second_moment, placement, block_counts, tokens, hidden_grad):
    expert_count = lax.axis_size("expert")
    dp_count = lax.axis_size("dp")
    chip_count = dp_count // 2
    block_total = weights.shape[0]
    span_rows = weights.shape[1]
    col_total = weights.shape[2]
    inputs = tokens[0, 0]
    row_total, wide = inputs.shape
    narrow = jnp.bfloat16
    own_count = expert_count * span_rows
    quarter = col_total // 4
    part_cols = 2 * quarter
    position = lax.axis_index("dp")
    chip, core = position // 2, position % 2
    place = jnp.stack([chip, core]).astype(jnp.int32)
    pick = (placement[:, None] == jnp.arange(block_total)[None, :]).astype(narrow)
    same = (placement[:, None] == placement[None, :]).astype(narrow)

    def exchange(values):
        return lax.all_to_all(values, "expert", split_axis=0, concat_axis=0, tiled=True)

    def choose(table, values):
        return jnp.einsum("jk,krc->jrc", table, values, preferred_element_type=jnp.float32).astype(narrow)

    def shift(value, step):
        pairs = [
            (2 * h + c, 2 * ((h + step) % chip_count) + c) for h in range(chip_count) for c in range(2)
        ]
        return lax.ppermute(value, "dp", pairs)

    def swap(value):
        return lax.ppermute(value, "dp", [(i, i ^ 1) for i in range(dp_count)])

    def halves(value):
        starts = range(0, value.shape[-1], 2 * quarter)
        even = jnp.concatenate([value[..., k : k + quarter] for k in starts], axis=-1)
        odd = jnp.concatenate([value[..., k + quarter : k + 2 * quarter] for k in starts], axis=-1)
        return jnp.where(core == 0, even, odd), jnp.where(core == 0, odd, even)

    def ordered(value):
        return jnp.concatenate(halves(value), axis=-1)

    def rows_of(value):
        return lax.optimization_barrier(value.reshape(own_count, value.shape[-1]))

    def add(*values):
        total = values[0].astype(jnp.float32)
        for value in values[1:]:
            total = total + value.astype(jnp.float32)
        return total.astype(narrow)

    live_mask = (jnp.arange(row_total) < BLOCK * block_counts[0, 0])[:, None]
    masked = jnp.where(live_mask, hidden_grad[0, 0], jnp.zeros((), narrow))
    hid_mine, hid_give = halves(masked)
    own_rows = exchange(choose(pick, ordered(weights))).reshape(own_count, col_total)
    mine, give = own_rows[:, :part_cols], own_rows[:, part_cols:]
    tok_theirs = swap(inputs)
    hid_theirs = swap(hid_give)
    plus_mine = shift(mine, 1)
    minus_mine = shift(mine, -1)
    theirs = swap(give)
    minus_theirs = shift(theirs, -1)
    plus_theirs = shift(theirs, 1)
    far_mine = shift(plus_mine, 1)
    far_theirs = shift(minus_theirs, -1)

    moments = ordered(jnp.concatenate([first_moment, second_moment], axis=1).astype(narrow))
    moments_sent, _ = lax.optimization_barrier((choose(pick, moments), own_rows))
    moments_here = exchange(moments_sent)

    turned = pl.pallas_call(
        turn_kernel,
        in_specs=in_vmem(2),
        out_specs=in_vmem(1)[0],
        out_shape=jax.ShapeDtypeStruct((wide, 2 * row_total), narrow),
        name="turn",
    )(inputs, tok_theirs)
    piece = jax.ShapeDtypeStruct((own_count, part_cols), narrow)
    partial = pl.pallas_call(
        partial_kernel,
        in_specs=in_smem() + in_vmem(8),
        out_specs=in_vmem(1)[0],
        out_shape=jax.ShapeDtypeStruct((2 * row_total, part_cols), jnp.float32),
        scratch_shapes=[pltpu.VMEM((3, 2 * own_count, part_cols), narrow)],
        name="partial",
    )(place, inputs, tok_theirs, mine, theirs, minus_mine, minus_theirs, plus_mine, plus_theirs)
    grad_proj, send_mine, last_mine = pl.pallas_call(
        project_kernel,
        in_specs=in_smem() + in_vmem(5) + in_any(3),
        out_specs=in_vmem(3),
        out_shape=[jax.ShapeDtypeStruct((2 * row_total, part_cols), narrow), piece, piece],
        scratch_shapes=[
            pltpu.VMEM((2 * own_count, part_cols), narrow),
            pltpu.VMEM((2 * row_total, 2 * own_count), narrow),
            pltpu.VMEM((own_count, 2 * row_total), narrow),
            pltpu.VMEM((own_count, 2 * row_total), narrow),
            pltpu.SemaphoreType.DMA((4,)),
        ],
        name="project",
    )(place, partial, hid_mine, hid_theirs, far_mine, far_theirs, inputs, tok_theirs, turned)
    got_plus = shift(send_mine, 1)
    early_mine = shift(last_mine, -1)
    send_theirs, next_mine, next_theirs, last_theirs, sum_mine, sum_theirs = pl.pallas_call(
        term_kernel,
        in_specs=in_smem() + in_vmem(2),
        out_specs=in_vmem(6),
        out_shape=[piece] * 6,
        name="terms",
    )(place, turned, grad_proj)
    got_minus = shift(send_theirs, -1)
    late_sent, next_theirs, moments_here = lax.optimization_barrier(
        (add(next_mine, got_plus), next_theirs, moments_here)
    )
    late_mine = shift(late_sent, 1)
    early_theirs = shift(next_theirs, 1)
    late_theirs = shift(add(last_theirs, got_minus), -1)
    total_mine = add(sum_mine, early_mine, late_mine)
    home_mine = exchange(total_mine.reshape(expert_count, span_rows, part_cols))
    total_other = swap(add(sum_theirs, early_theirs, late_theirs))
    home_other = exchange(total_other.reshape(expert_count, span_rows, part_cols))
    sums = jnp.concatenate([choose(same, home_mine), choose(same, home_other)], axis=-1)
    grad_rows = rows_of(exchange(sums))
    bands = chip_count
    band = own_count // bands
    spec = pl.BlockSpec((band, col_total), lambda i: (i, 0))
    out_spec = pl.BlockSpec((1, band, col_total), lambda i: (0, i, 0))
    shape = (1, own_count, col_total)
    return pl.pallas_call(
        adam_kernel,
        grid=(bands,),
        in_specs=in_smem() + [spec] * 4,
        out_specs=[out_spec] * 3,
        out_shape=[
            jax.ShapeDtypeStruct(shape, narrow),
            jax.ShapeDtypeStruct(shape, jnp.float32),
            jax.ShapeDtypeStruct(shape, jnp.float32),
        ],
        name="adam",
    )(
        place, own_rows, rows_of(moments_here[:, :span_rows]), rows_of(moments_here[:, span_rows:]),
        grad_rows,
    )


def solution(mesh):
    in_specs = (
        P(None, ("dp", "expert"), None),
        P(None, ("dp", "expert"), None),
        P(None, ("dp", "expert"), None),
        P(),
        P("dp", "expert"),
        P("dp", "expert", None, None),
        P("dp", "expert", None, None),
    )
    out_specs = (P("expert", "dp", None), P("expert", "dp", None), P("expert", "dp", None))

    return jax.shard_map(on_device, mesh=mesh, in_specs=in_specs, out_specs=out_specs, check_vma=False)
```

```python
import jax
import jax.numpy as jnp
from jax import lax
from jax.experimental import pallas as pl
from jax.experimental.pallas import tpu as pltpu
from jax.sharding import PartitionSpec as P


BLOCK = 128


beta_first = 0.9
beta_second = 0.95
learning_rate = 0.001
weight_decay = 0.1
adam_epsilon = 1e-08
adam_steps = 10.0


def adam_update(params, first_moment, second_moment, gradient):
    moment_one = beta_first * first_moment + (1.0 - beta_first) * gradient
    moment_two = beta_second * second_moment + (1.0 - beta_second) * gradient * gradient
    correct_one = 1.0 - beta_first**adam_steps
    correct_two = 1.0 - beta_second**adam_steps
    params_full = params.astype(jnp.float32)
    step_size = (
        moment_one / correct_one / (jnp.sqrt(moment_two / correct_two) + adam_epsilon)
        + weight_decay * params_full
    )
    return ((params_full - learning_rate * step_size).astype(jnp.bfloat16), moment_one, moment_two)


def grad_halves(projected, upstream):
    half_width = projected.shape[1] // 2
    gate_part = projected[:, :half_width]
    upward = projected[:, half_width:]
    sigmoid_gate = jax.nn.sigmoid(gate_part)
    masked = upstream.astype(jnp.float32)
    grad_gate = masked * upward * sigmoid_gate * (1.0 + gate_part * (1.0 - sigmoid_gate))
    grad_upward = masked * gate_part * sigmoid_gate
    return grad_gate.astype(jnp.bfloat16), grad_upward.astype(jnp.bfloat16)


def term_rows(turned_ref, grad_ref, start, count):
    rows = turned_ref[pl.ds(pl.multiple_of(start, 16), count), :]
    return jnp.dot(rows, grad_ref[...], preferred_element_type=jnp.float32).astype(jnp.bfloat16)


def piece_start(place, step, side, count):
    return pl.multiple_of((2 * ((place[0] + step) % 4) + (place[1] + side) % 2) * count, 16)


def block_start(place, step, count):
    return pl.multiple_of(((place[0] + step) % 4) * 2 * count, 128)


def join(place, block, mine, theirs):
    count = mine.shape[0]
    core = place[1]
    block[pl.ds(pl.multiple_of(core * count, 16), count), :] = mine[...]
    block[pl.ds(pl.multiple_of((1 - core) * count, 16), count), :] = theirs[...]


def partial_kernel(place, tok_mine, tok_theirs, *rest):
    pieces, partial, block = rest[:6], rest[6], rest[7]
    count = pieces[0].shape[0]
    half = tok_mine.shape[0]
    for slot in range(3):
        join(place, block.at[slot], pieces[2 * slot], pieces[2 * slot + 1])
    for low, tok in ((0, tok_mine), (half, tok_theirs)):
        total = None
        for slot, step in enumerate((0, 1, 3)):
            part = jnp.dot(
                tok[:, pl.ds(block_start(place, step, count), 2 * count)],
                block[slot],
                preferred_element_type=jnp.float32,
            )
            total = part if total is None else total + part
        partial[low : low + half, :] = total


def project_kernel(
    place, partial, hid_mine, hid_theirs, piece_mine, piece_theirs, tok_mine, tok_theirs, turned,
    grad_ref, far_mine, last_mine, block, far_tok, far_rows, last_rows, sems,
):
    count = piece_mine.shape[0]
    half = hid_mine.shape[0]
    lanes = pl.ds(block_start(place, 2, count), 2 * count)
    copies = [
        pltpu.make_async_copy(tok_mine.at[:, lanes], far_tok.at[0:half], sems.at[0]),
        pltpu.make_async_copy(tok_theirs.at[:, lanes], far_tok.at[half : 2 * half], sems.at[1]),
        pltpu.make_async_copy(
            turned.at[pl.ds(piece_start(place, 2, 0, count), count)], far_rows, sems.at[2]
        ),
        pltpu.make_async_copy(
            turned.at[pl.ds(piece_start(place, 3, 0, count), count)], last_rows, sems.at[3]
        ),
    ]
    for copy in copies:
        copy.start()
    join(place, block, piece_mine, piece_theirs)
    width = block.shape[1] // 2
    copies[0].wait()
    copies[1].wait()
    for hid, low in ((hid_mine, 0), (hid_theirs, half)):
        projected = partial[low : low + half, :] + jnp.dot(
            far_tok[low : low + half, :], block[...], preferred_element_type=jnp.float32
        )
        grad_gate, grad_up = grad_halves(projected, hid[...])
        grad_ref[low : low + half, :width] = grad_gate
        grad_ref[low : low + half, width:] = grad_up
    copies[2].wait()
    copies[3].wait()
    grads = grad_ref[...]
    far_mine[...] = jnp.dot(far_rows[...], grads, preferred_element_type=jnp.float32).astype(jnp.bfloat16)
    last_mine[...] = jnp.dot(last_rows[...], grads, preferred_element_type=jnp.float32).astype(jnp.bfloat16)


def turn_kernel(tok_mine, tok_theirs, turned):
    half, wide = tok_mine.shape
    for low, tok in ((0, tok_mine), (half, tok_theirs)):
        for begin in range(0, wide, 512):
            turned[begin : begin + 512, low : low + half] = tok[:, begin : begin + 512].T


def term_kernel(place, turned, grad_ref, *outs):
    count = outs[0].shape[0]
    for slot, (step, side) in enumerate(((2, 1), (1, 0), (1, 1), (3, 1), (0, 0), (0, 1))):
        outs[slot][...] = term_rows(turned, grad_ref, piece_start(place, step, side, count), count)


def adam_kernel(place, params, first, second, gradient, updated, moment_one, moment_two):
    lanes = params.shape[1] // 4
    for kind in range(2):
        for side in range(2):
            read = pl.ds((2 * side + kind) * lanes, lanes)
            into = pl.ds(pl.multiple_of((2 * kind + (place[1] + side) % 2) * lanes, 128), lanes)
            new_params, new_one, new_two = adam_update(
                params[:, read],
                first[:, read].astype(jnp.float32),
                second[:, read].astype(jnp.float32),
                gradient[:, read].astype(jnp.float32),
            )
            updated[0, :, into] = new_params
            moment_one[0, :, into] = new_one
            moment_two[0, :, into] = new_two


def in_vmem(count):
    return [pl.BlockSpec(memory_space=pltpu.VMEM) for _ in range(count)]


def in_smem():
    return [pl.BlockSpec(memory_space=pltpu.SMEM)]


def in_any(count):
    return [pl.BlockSpec(memory_space=pl.ANY) for _ in range(count)]


def on_device(weights, first_moment, second_moment, placement, block_counts, tokens, hidden_grad):
    expert_count = lax.axis_size("expert")
    dp_count = lax.axis_size("dp")
    chip_count = dp_count // 2
    block_total = weights.shape[0]
    span_rows = weights.shape[1]
    col_total = weights.shape[2]
    inputs = tokens[0, 0]
    row_total, wide = inputs.shape
    narrow = jnp.bfloat16
    own_count = expert_count * span_rows
    quarter = col_total // 4
    part_cols = 2 * quarter
    position = lax.axis_index("dp")
    chip, core = position // 2, position % 2
    place = jnp.stack([chip, core]).astype(jnp.int32)
    pick = (placement[:, None] == jnp.arange(block_total)[None, :]).astype(narrow)
    same = (placement[:, None] == placement[None, :]).astype(narrow)

    def exchange(values):
        return lax.all_to_all(values, "expert", split_axis=0, concat_axis=0, tiled=True)

    def choose(table, values):
        return jnp.einsum("jk,krc->jrc", table, values, preferred_element_type=jnp.float32).astype(narrow)

    def shift(value, step):
        pairs = [
            (2 * h + c, 2 * ((h + step) % chip_count) + c) for h in range(chip_count) for c in range(2)
        ]
        return lax.ppermute(value, "dp", pairs)

    def swap(value):
        return lax.ppermute(value, "dp", [(i, i ^ 1) for i in range(dp_count)])

    def halves(value):
        starts = range(0, value.shape[-1], 2 * quarter)
        even = jnp.concatenate([value[..., k : k + quarter] for k in starts], axis=-1)
        odd = jnp.concatenate([value[..., k + quarter : k + 2 * quarter] for k in starts], axis=-1)
        return jnp.where(core == 0, even, odd), jnp.where(core == 0, odd, even)

    def ordered(value):
        return jnp.concatenate(halves(value), axis=-1)

    def rows_of(value):
        return lax.optimization_barrier(value.reshape(own_count, value.shape[-1]))

    def add(*values):
        total = values[0].astype(jnp.float32)
        for value in values[1:]:
            total = total + value.astype(jnp.float32)
        return total.astype(narrow)

    live_mask = (jnp.arange(row_total) < BLOCK * block_counts[0, 0])[:, None]
    masked = jnp.where(live_mask, hidden_grad[0, 0], jnp.zeros((), narrow))
    hid_mine, hid_give = halves(masked)
    arrived = exchange(choose(pick, ordered(weights)))
    own_rows = arrived.reshape(own_count, col_total)
    mine, give = own_rows[:, :part_cols], own_rows[:, part_cols:]
    tok_theirs = swap(inputs)
    hid_theirs = swap(hid_give)
    plus_mine = shift(mine, 1)
    minus_mine = shift(mine, -1)
    theirs = swap(give)
    minus_theirs = shift(theirs, -1)
    plus_theirs = shift(theirs, 1)
    far_mine = shift(plus_mine, 1)
    far_theirs = shift(minus_theirs, -1)

    moments_sent = choose(
        pick, ordered(jnp.concatenate([first_moment, second_moment], axis=1).astype(narrow))
    )
    moments_here = exchange(moments_sent)

    turned = pl.pallas_call(
        turn_kernel,
        in_specs=in_vmem(2),
        out_specs=in_vmem(1)[0],
        out_shape=jax.ShapeDtypeStruct((wide, 2 * row_total), narrow),
        name="turn",
    )(inputs, tok_theirs)
    piece = jax.ShapeDtypeStruct((own_count, part_cols), narrow)
    partial = pl.pallas_call(
        partial_kernel,
        in_specs=in_smem() + in_vmem(8),
        out_specs=in_vmem(1)[0],
        out_shape=jax.ShapeDtypeStruct((2 * row_total, part_cols), jnp.float32),
        scratch_shapes=[pltpu.VMEM((3, 2 * own_count, part_cols), narrow)],
        name="partial",
    )(place, inputs, tok_theirs, mine, theirs, minus_mine, minus_theirs, plus_mine, plus_theirs)
    grad_proj, send_mine, last_mine = pl.pallas_call(
        project_kernel,
        in_specs=in_smem() + in_vmem(5) + in_any(3),
        out_specs=in_vmem(3),
        out_shape=[jax.ShapeDtypeStruct((2 * row_total, part_cols), narrow), piece, piece],
        scratch_shapes=[
            pltpu.VMEM((2 * own_count, part_cols), narrow),
            pltpu.VMEM((2 * row_total, 2 * own_count), narrow),
            pltpu.VMEM((own_count, 2 * row_total), narrow),
            pltpu.VMEM((own_count, 2 * row_total), narrow),
            pltpu.SemaphoreType.DMA((4,)),
        ],
        name="project",
    )(place, partial, hid_mine, hid_theirs, far_mine, far_theirs, inputs, tok_theirs, turned)
    got_plus = shift(send_mine, 1)
    early_mine = shift(last_mine, -1)
    send_theirs, next_mine, next_theirs, last_theirs, sum_mine, sum_theirs = pl.pallas_call(
        term_kernel,
        in_specs=in_smem() + in_vmem(2),
        out_specs=in_vmem(6),
        out_shape=[piece] * 6,
        name="terms",
    )(place, turned, grad_proj)
    got_minus = shift(send_theirs, -1)
    late_sent, next_theirs, moments_here = lax.optimization_barrier(
        (add(next_mine, got_plus), next_theirs, moments_here)
    )
    late_mine = shift(late_sent, 1)
    early_theirs = shift(next_theirs, 1)
    late_theirs = shift(add(last_theirs, got_minus), -1)
    total_mine = add(sum_mine, early_mine, late_mine)
    home_mine = exchange(total_mine.reshape(expert_count, span_rows, part_cols))
    total_other = swap(add(sum_theirs, early_theirs, late_theirs))
    home_other = exchange(total_other.reshape(expert_count, span_rows, part_cols))
    sums = jnp.concatenate([choose(same, home_mine), choose(same, home_other)], axis=-1)
    grad_rows = rows_of(exchange(sums))
    bands = chip_count
    band = own_count // bands
    spec = pl.BlockSpec((band, col_total), lambda i: (i, 0))
    out_spec = pl.BlockSpec((1, band, col_total), lambda i: (0, i, 0))
    shape = (1, own_count, col_total)
    return pl.pallas_call(
        adam_kernel,
        grid=(bands,),
        in_specs=in_smem() + [spec] * 4,
        out_specs=[out_spec] * 3,
        out_shape=[
            jax.ShapeDtypeStruct(shape, narrow),
            jax.ShapeDtypeStruct(shape, jnp.float32),
            jax.ShapeDtypeStruct(shape, jnp.float32),
        ],
        name="adam",
    )(
        place, own_rows, rows_of(moments_here[:, :span_rows]), rows_of(moments_here[:, span_rows:]),
        grad_rows,
    )


def solution(mesh):
    in_specs = (
        P(None, ("dp", "expert"), None),
        P(None, ("dp", "expert"), None),
        P(None, ("dp", "expert"), None),
        P(),
        P("dp", "expert"),
        P("dp", "expert", None, None),
        P("dp", "expert", None, None),
    )
    out_specs = (P("expert", "dp", None), P("expert", "dp", None), P("expert", "dp", None))

    return jax.shard_map(on_device, mesh=mesh, in_specs=in_specs, out_specs=out_specs, check_vma=False)
```

```python
import jax
import jax.numpy as jnp
from jax import lax
from jax.experimental import pallas as pl
from jax.experimental.pallas import tpu as pltpu
from jax.sharding import PartitionSpec as P


BLOCK = 128


beta_first = 0.9
beta_second = 0.95
learning_rate = 0.001
weight_decay = 0.1
adam_epsilon = 1e-08
adam_steps = 10.0


def adam_update(params, first_moment, second_moment, gradient):
    moment_one = beta_first * first_moment + (1.0 - beta_first) * gradient
    moment_two = beta_second * second_moment + (1.0 - beta_second) * gradient * gradient
    correct_one = 1.0 - beta_first**adam_steps
    correct_two = 1.0 - beta_second**adam_steps
    params_full = params.astype(jnp.float32)
    step_size = (
        moment_one / correct_one / (jnp.sqrt(moment_two / correct_two) + adam_epsilon)
        + weight_decay * params_full
    )
    return ((params_full - learning_rate * step_size).astype(jnp.bfloat16), moment_one, moment_two)


def grad_halves(projected, upstream):
    half_width = projected.shape[1] // 2
    gate_part = projected[:, :half_width]
    upward = projected[:, half_width:]
    sigmoid_gate = jax.nn.sigmoid(gate_part)
    masked = upstream.astype(jnp.float32)
    grad_gate = masked * upward * sigmoid_gate * (1.0 + gate_part * (1.0 - sigmoid_gate))
    grad_upward = masked * gate_part * sigmoid_gate
    return grad_gate.astype(jnp.bfloat16), grad_upward.astype(jnp.bfloat16)


def term_rows(turned_ref, grad_ref, start, count):
    rows = turned_ref[pl.ds(pl.multiple_of(start, 16), count), :]
    return jnp.dot(rows, grad_ref[...], preferred_element_type=jnp.float32).astype(jnp.bfloat16)


def piece_start(place, step, side, count):
    return pl.multiple_of((2 * ((place[0] + step) % 4) + (place[1] + side) % 2) * count, 16)


def block_start(place, step, count):
    return pl.multiple_of(((place[0] + step) % 4) * 2 * count, 128)


def join(place, block, mine, theirs):
    count = mine.shape[0]
    core = place[1]
    block[pl.ds(pl.multiple_of(core * count, 16), count), :] = mine[...]
    block[pl.ds(pl.multiple_of((1 - core) * count, 16), count), :] = theirs[...]


def partial_kernel(place, tok_mine, tok_theirs, *rest):
    pieces, partial, block = rest[:6], rest[6], rest[7]
    count = pieces[0].shape[0]
    half = tok_mine.shape[0]
    for slot in range(3):
        join(place, block.at[slot], pieces[2 * slot], pieces[2 * slot + 1])
    for low, tok in ((0, tok_mine), (half, tok_theirs)):
        total = None
        for slot, step in enumerate((0, 1, 3)):
            part = jnp.dot(
                tok[:, pl.ds(block_start(place, step, count), 2 * count)],
                block[slot],
                preferred_element_type=jnp.float32,
            )
            total = part if total is None else total + part
        partial[low : low + half, :] = total


def project_kernel(
    place, partial, hid_mine, hid_theirs, piece_mine, piece_theirs, tok_mine, tok_theirs, turned,
    grad_ref, far_mine, far_theirs, block, far_tok, far_rows, other_rows, sems,
):
    count = piece_mine.shape[0]
    half = hid_mine.shape[0]
    lanes = pl.ds(block_start(place, 2, count), 2 * count)
    copies = [
        pltpu.make_async_copy(tok_mine.at[:, lanes], far_tok.at[0:half], sems.at[0]),
        pltpu.make_async_copy(tok_theirs.at[:, lanes], far_tok.at[half : 2 * half], sems.at[1]),
        pltpu.make_async_copy(
            turned.at[pl.ds(piece_start(place, 2, 0, count), count)], far_rows, sems.at[2]
        ),
        pltpu.make_async_copy(
            turned.at[pl.ds(piece_start(place, 2, 1, count), count)], other_rows, sems.at[3]
        ),
    ]
    for copy in copies:
        copy.start()
    join(place, block, piece_mine, piece_theirs)
    width = block.shape[1] // 2
    copies[0].wait()
    copies[1].wait()
    for hid, low in ((hid_mine, 0), (hid_theirs, half)):
        projected = partial[low : low + half, :] + jnp.dot(
            far_tok[low : low + half, :], block[...], preferred_element_type=jnp.float32
        )
        grad_gate, grad_up = grad_halves(projected, hid[...])
        grad_ref[low : low + half, :width] = grad_gate
        grad_ref[low : low + half, width:] = grad_up
    copies[2].wait()
    copies[3].wait()
    grads = grad_ref[...]
    far_mine[...] = jnp.dot(far_rows[...], grads, preferred_element_type=jnp.float32).astype(jnp.bfloat16)
    far_theirs[...] = jnp.dot(other_rows[...], grads, preferred_element_type=jnp.float32).astype(jnp.bfloat16)


def turn_kernel(tok_mine, tok_theirs, turned):
    half, wide = tok_mine.shape
    for low, tok in ((0, tok_mine), (half, tok_theirs)):
        for begin in range(0, wide, 512):
            turned[begin : begin + 512, low : low + half] = tok[:, begin : begin + 512].T


def term_kernel(place, turned, grad_ref, *outs):
    count = outs[0].shape[0]
    for slot, (step, side) in enumerate(((1, 0), (1, 1), (3, 0), (3, 1), (0, 0), (0, 1))):
        outs[slot][...] = term_rows(turned, grad_ref, piece_start(place, step, side, count), count)


def adam_kernel(place, params, first, second, gradient, updated, moment_one, moment_two):
    lanes = params.shape[1] // 4
    for kind in range(2):
        for side in range(2):
            read = pl.ds((2 * side + kind) * lanes, lanes)
            into = pl.ds(pl.multiple_of((2 * kind + (place[1] + side) % 2) * lanes, 128), lanes)
            new_params, new_one, new_two = adam_update(
                params[:, read],
                first[:, read].astype(jnp.float32),
                second[:, read].astype(jnp.float32),
                gradient[:, read].astype(jnp.float32),
            )
            updated[0, :, into] = new_params
            moment_one[0, :, into] = new_one
            moment_two[0, :, into] = new_two


def in_vmem(count):
    return [pl.BlockSpec(memory_space=pltpu.VMEM) for _ in range(count)]


def in_smem():
    return [pl.BlockSpec(memory_space=pltpu.SMEM)]


def in_any(count):
    return [pl.BlockSpec(memory_space=pl.ANY) for _ in range(count)]


def on_device(weights, first_moment, second_moment, placement, block_counts, tokens, hidden_grad):
    expert_count = lax.axis_size("expert")
    dp_count = lax.axis_size("dp")
    chip_count = dp_count // 2
    block_total = weights.shape[0]
    span_rows = weights.shape[1]
    col_total = weights.shape[2]
    inputs = tokens[0, 0]
    row_total, wide = inputs.shape
    narrow = jnp.bfloat16
    own_count = expert_count * span_rows
    quarter = col_total // 4
    part_cols = 2 * quarter
    position = lax.axis_index("dp")
    chip, core = position // 2, position % 2
    place = jnp.stack([chip, core]).astype(jnp.int32)
    pick = (placement[:, None] == jnp.arange(block_total)[None, :]).astype(narrow)
    same = (placement[:, None] == placement[None, :]).astype(narrow)

    def exchange(values):
        return lax.all_to_all(values, "expert", split_axis=0, concat_axis=0, tiled=True)

    def choose(table, values):
        return jnp.einsum("jk,krc->jrc", table, values, preferred_element_type=jnp.float32).astype(narrow)

    def shift(value, step):
        pairs = [
            (2 * h + c, 2 * ((h + step) % chip_count) + c) for h in range(chip_count) for c in range(2)
        ]
        return lax.ppermute(value, "dp", pairs)

    def swap(value):
        return lax.ppermute(value, "dp", [(i, i ^ 1) for i in range(dp_count)])

    def halves(value):
        starts = range(0, value.shape[-1], 2 * quarter)
        even = jnp.concatenate([value[..., k : k + quarter] for k in starts], axis=-1)
        odd = jnp.concatenate([value[..., k + quarter : k + 2 * quarter] for k in starts], axis=-1)
        return jnp.where(core == 0, even, odd), jnp.where(core == 0, odd, even)

    def ordered(value):
        return jnp.concatenate(halves(value), axis=-1)

    def rows_of(value):
        return lax.optimization_barrier(value.reshape(own_count, value.shape[-1]))

    def add(*values):
        total = values[0].astype(jnp.float32)
        for value in values[1:]:
            total = total + value.astype(jnp.float32)
        return total.astype(narrow)

    live_mask = (jnp.arange(row_total) < BLOCK * block_counts[0, 0])[:, None]
    masked = jnp.where(live_mask, hidden_grad[0, 0], jnp.zeros((), narrow))
    hid_mine, hid_give = halves(masked)
    arrived = exchange(choose(pick, ordered(weights)))
    own_rows = arrived.reshape(own_count, col_total)
    mine, give = own_rows[:, :part_cols], own_rows[:, part_cols:]
    tok_theirs = swap(inputs)
    hid_theirs = swap(hid_give)
    plus_mine = shift(mine, 1)
    minus_mine = shift(mine, -1)
    theirs = swap(give)
    minus_theirs = shift(theirs, -1)
    plus_theirs = shift(theirs, 1)
    far_mine = shift(plus_mine, 1)
    far_theirs = shift(minus_theirs, -1)

    stored = ordered(jnp.concatenate([first_moment, second_moment], axis=1).astype(narrow))
    group = expert_count // 2
    beside = lax.ppermute(stored, "expert", [(e, (e + group) % expert_count) for e in range(expert_count)])
    upper = lax.axis_index("expert") // group
    low = jnp.where(upper == 0, stored, beside)
    high = jnp.where(upper == 0, beside, stored)
    group_pick = lax.dynamic_slice_in_dim(pick, upper * group, group, 0)
    moments_sent = choose(group_pick, jnp.concatenate([low, high], axis=1))
    moments_here = lax.all_to_all(
        moments_sent, "expert", split_axis=0, concat_axis=0, tiled=True,
        axis_index_groups=[list(range(group)), list(range(group, expert_count))],
    )

    turned = pl.pallas_call(
        turn_kernel,
        in_specs=in_vmem(2),
        out_specs=in_vmem(1)[0],
        out_shape=jax.ShapeDtypeStruct((wide, 2 * row_total), narrow),
        name="turn",
    )(inputs, tok_theirs)
    piece = jax.ShapeDtypeStruct((own_count, part_cols), narrow)
    partial = pl.pallas_call(
        partial_kernel,
        in_specs=in_smem() + in_vmem(8),
        out_specs=in_vmem(1)[0],
        out_shape=jax.ShapeDtypeStruct((2 * row_total, part_cols), jnp.float32),
        scratch_shapes=[pltpu.VMEM((3, 2 * own_count, part_cols), narrow)],
        name="partial",
    )(place, inputs, tok_theirs, mine, theirs, minus_mine, minus_theirs, plus_mine, plus_theirs)
    grad_proj, send_mine, send_theirs = pl.pallas_call(
        project_kernel,
        in_specs=in_smem() + in_vmem(5) + in_any(3),
        out_specs=in_vmem(3),
        out_shape=[jax.ShapeDtypeStruct((2 * row_total, part_cols), narrow), piece, piece],
        scratch_shapes=[
            pltpu.VMEM((2 * own_count, part_cols), narrow),
            pltpu.VMEM((2 * row_total, 2 * own_count), narrow),
            pltpu.VMEM((own_count, 2 * row_total), narrow),
            pltpu.VMEM((own_count, 2 * row_total), narrow),
            pltpu.SemaphoreType.DMA((4,)),
        ],
        name="project",
    )(place, partial, hid_mine, hid_theirs, far_mine, far_theirs, inputs, tok_theirs, turned)
    got_plus = shift(send_mine, 1)
    got_minus = shift(send_theirs, -1)
    next_mine, next_theirs, last_mine, last_theirs, sum_mine, sum_theirs = pl.pallas_call(
        term_kernel,
        in_specs=in_smem() + in_vmem(2),
        out_specs=in_vmem(6),
        out_shape=[piece] * 6,
        name="terms",
    )(place, turned, grad_proj)
    early_theirs = shift(next_theirs, 1)
    early_mine = shift(last_mine, -1)
    late_mine = shift(add(next_mine, got_plus), 1)
    late_theirs = shift(add(last_theirs, got_minus), -1)
    late_mine, late_theirs, moments_here = lax.optimization_barrier((late_mine, late_theirs, moments_here))
    total_other = swap(add(sum_theirs, early_theirs, late_theirs))
    total = jnp.concatenate([add(sum_mine, early_mine, late_mine), total_other], axis=1)
    home = exchange(total.reshape(expert_count, span_rows, col_total))

    def moment_rows(kind):
        sides = [
            moments_here[:, (2 * side + kind) * span_rows : (2 * side + kind + 1) * span_rows]
            for side in range(2)
        ]
        return rows_of(jnp.concatenate(sides, axis=0))

    grad_rows = rows_of(exchange(choose(same, home)))
    bands = chip_count
    band = own_count // bands
    spec = pl.BlockSpec((band, col_total), lambda i: (i, 0))
    out_spec = pl.BlockSpec((1, band, col_total), lambda i: (0, i, 0))
    shape = (1, own_count, col_total)
    return pl.pallas_call(
        adam_kernel,
        grid=(bands,),
        in_specs=in_smem() + [spec] * 4,
        out_specs=[out_spec] * 3,
        out_shape=[
            jax.ShapeDtypeStruct(shape, narrow),
            jax.ShapeDtypeStruct(shape, jnp.float32),
            jax.ShapeDtypeStruct(shape, jnp.float32),
        ],
        name="adam",
    )(
        place, own_rows, moment_rows(0), moment_rows(1), grad_rows,
    )


def solution(mesh):
    in_specs = (
        P(None, ("dp", "expert"), None),
        P(None, ("dp", "expert"), None),
        P(None, ("dp", "expert"), None),
        P(),
        P("dp", "expert"),
        P("dp", "expert", None, None),
        P("dp", "expert", None, None),
    )
    out_specs = (P("expert", "dp", None), P("expert", "dp", None), P("expert", "dp", None))

    return jax.shard_map(on_device, mesh=mesh, in_specs=in_specs, out_specs=out_specs, check_vma=False)
```

```python
import jax
import jax.numpy as jnp
from jax import lax
from jax.experimental import pallas as pl
from jax.experimental.pallas import tpu as pltpu
from jax.sharding import PartitionSpec as P


BLOCK = 128
MEBI = 1 << 20


beta_first = 0.9
beta_second = 0.95
learning_rate = 0.001
weight_decay = 0.1
adam_epsilon = 1e-08
adam_steps = 10.0


def adam_update(params, first_moment, second_moment, gradient):
    moment_one = beta_first * first_moment + (1.0 - beta_first) * gradient
    moment_two = beta_second * second_moment + (1.0 - beta_second) * gradient * gradient
    correct_one = 1.0 - beta_first**adam_steps
    correct_two = 1.0 - beta_second**adam_steps
    params_full = params.astype(jnp.float32)
    step_size = (
        moment_one / correct_one / (jnp.sqrt(moment_two / correct_two) + adam_epsilon)
        + weight_decay * params_full
    )
    return ((params_full - learning_rate * step_size).astype(jnp.bfloat16), moment_one, moment_two)


def grad_halves(projected, upstream):
    half_width = projected.shape[1] // 2
    gate_part = projected[:, :half_width]
    upward = projected[:, half_width:]
    sigmoid_gate = jax.nn.sigmoid(gate_part)
    masked = upstream.astype(jnp.float32)
    grad_gate = masked * upward * sigmoid_gate * (1.0 + gate_part * (1.0 - sigmoid_gate))
    grad_upward = masked * gate_part * sigmoid_gate
    return grad_gate.astype(jnp.bfloat16), grad_upward.astype(jnp.bfloat16)


def term_rows(turned_ref, grad_ref, start, count):
    rows = turned_ref[pl.ds(pl.multiple_of(start, 16), count), :]
    return jnp.dot(rows, grad_ref[...], preferred_element_type=jnp.float32).astype(jnp.bfloat16)


def piece_start(place, step, side, count):
    return pl.multiple_of((2 * ((place[0] + step) % 4) + (place[1] + side) % 2) * count, 16)


def block_start(place, step, count):
    return pl.multiple_of(((place[0] + step) % 4) * 2 * count, 128)


def join(place, block, mine, theirs):
    count = mine.shape[0]
    core = place[1]
    block[pl.ds(pl.multiple_of(core * count, 16), count), :] = mine[...]
    block[pl.ds(pl.multiple_of((1 - core) * count, 16), count), :] = theirs[...]


def partial_kernel(place, tok_mine, tok_theirs, *rest):
    pieces, partial, block = rest[:6], rest[6], rest[7]
    count = pieces[0].shape[0]
    half = tok_mine.shape[0]
    for slot in range(3):
        join(place, block.at[slot], pieces[2 * slot], pieces[2 * slot + 1])
    for low, tok in ((0, tok_mine), (half, tok_theirs)):
        total = None
        for slot, step in enumerate((0, 1, 3)):
            part = jnp.dot(
                tok[:, pl.ds(block_start(place, step, count), 2 * count)],
                block[slot],
                preferred_element_type=jnp.float32,
            )
            total = part if total is None else total + part
        partial[low : low + half, :] = total


def project_kernel(
    place, partial, hid_mine, hid_theirs, piece_mine, piece_theirs, far_tok, far_turned,
    grad_ref, far_mine, far_theirs, block,
):
    count = piece_mine.shape[0]
    half = hid_mine.shape[0]
    width = block.shape[1] // 2
    join(place, block, piece_mine, piece_theirs)
    for hid, low in ((hid_mine, 0), (hid_theirs, half)):
        projected = partial[low : low + half, :] + jnp.dot(
            far_tok[low : low + half, :], block[...], preferred_element_type=jnp.float32
        )
        grad_gate, grad_up = grad_halves(projected, hid[...])
        grad_ref[low : low + half, :width] = grad_gate
        grad_ref[low : low + half, width:] = grad_up
    for out, core in ((far_mine, place[1]), (far_theirs, 1 - place[1])):
        out[...] = term_rows(far_turned, grad_ref, core * count, count)


def turn_kernel(place, tok_mine, tok_theirs, turned, far_tok, far_turned):
    half, wide = tok_mine.shape
    far = far_tok.shape[1]
    begin = pl.multiple_of(((place[0] + 2) % 4) * far, 128)
    for low, tok in ((0, tok_mine), (half, tok_theirs)):
        for step in range(0, wide, 512):
            turned[step : step + 512, low : low + half] = tok[:, step : step + 512].T
        far_tok[low : low + half, :] = tok[:, pl.ds(begin, far)]
    far_turned[...] = turned[pl.ds(begin, far), :]


def term_kernel(place, turned, grad_ref, *outs):
    count = outs[0].shape[0]
    for slot, (step, side) in enumerate(((1, 0), (1, 1), (3, 0), (3, 1), (0, 0), (0, 1))):
        outs[slot][...] = term_rows(turned, grad_ref, piece_start(place, step, side, count), count)


def adam_kernel(place, params, first, second, gradient, updated, moment_one, moment_two):
    lanes = params.shape[1] // 4
    for kind in range(2):
        for side in range(2):
            read = pl.ds((2 * side + kind) * lanes, lanes)
            into = pl.ds(pl.multiple_of((2 * kind + (place[1] + side) % 2) * lanes, 128), lanes)
            new_params, new_one, new_two = adam_update(
                params[:, read],
                first[:, read].astype(jnp.float32),
                second[:, read].astype(jnp.float32),
                gradient[:, read].astype(jnp.float32),
            )
            updated[0, :, into] = new_params
            moment_one[0, :, into] = new_one
            moment_two[0, :, into] = new_two


def in_vmem(count):
    return [pl.BlockSpec(memory_space=pltpu.VMEM) for _ in range(count)]


def in_smem():
    return [pl.BlockSpec(memory_space=pltpu.SMEM)]


def on_device(weights, first_moment, second_moment, placement, block_counts, tokens, hidden_grad):
    expert_count = lax.axis_size("expert")
    dp_count = lax.axis_size("dp")
    chip_count = dp_count // 2
    block_total = weights.shape[0]
    span_rows = weights.shape[1]
    col_total = weights.shape[2]
    inputs = tokens[0, 0]
    row_total, wide = inputs.shape
    narrow = jnp.bfloat16
    own_count = expert_count * span_rows
    quarter = col_total // 4
    part_cols = 2 * quarter
    position = lax.axis_index("dp")
    chip, core = position // 2, position % 2
    place = jnp.stack([chip, core]).astype(jnp.int32)
    pick = (placement[:, None] == jnp.arange(block_total)[None, :]).astype(narrow)
    same = (placement[:, None] == placement[None, :]).astype(narrow)

    def exchange(values):
        return lax.all_to_all(values, "expert", split_axis=0, concat_axis=0, tiled=True)

    def choose(table, values):
        return jnp.einsum("jk,krc->jrc", table, values, preferred_element_type=jnp.float32).astype(narrow)

    def shift(value, step):
        pairs = [
            (2 * h + c, 2 * ((h + step) % chip_count) + c) for h in range(chip_count) for c in range(2)
        ]
        return lax.ppermute(value, "dp", pairs)

    def swap(value):
        return lax.ppermute(value, "dp", [(i, i ^ 1) for i in range(dp_count)])

    def halves(value):
        starts = range(0, value.shape[-1], 2 * quarter)
        even = jnp.concatenate([value[..., k : k + quarter] for k in starts], axis=-1)
        odd = jnp.concatenate([value[..., k + quarter : k + 2 * quarter] for k in starts], axis=-1)
        return jnp.where(core == 0, even, odd), jnp.where(core == 0, odd, even)

    def ordered(value):
        return jnp.concatenate(halves(value), axis=-1)

    def rows_of(value):
        return lax.optimization_barrier(value.reshape(own_count, value.shape[-1]))

    def add(*values):
        total = values[0].astype(jnp.float32)
        for value in values[1:]:
            total = total + value.astype(jnp.float32)
        return total.astype(narrow)

    live_mask = (jnp.arange(row_total) < BLOCK * block_counts[0, 0])[:, None]
    masked = jnp.where(live_mask, hidden_grad[0, 0], jnp.zeros((), narrow))
    hid_mine, hid_give = halves(masked)
    arrived = exchange(choose(pick, ordered(weights)))
    own_rows = arrived.reshape(own_count, col_total)
    mine, give = own_rows[:, :part_cols], own_rows[:, part_cols:]
    tok_theirs = swap(inputs)
    hid_theirs = swap(hid_give)
    plus_mine = shift(mine, 1)
    minus_mine = shift(mine, -1)
    theirs = swap(give)
    minus_theirs = shift(theirs, -1)
    plus_theirs = shift(theirs, 1)
    far_mine = shift(plus_mine, 1)
    far_theirs = shift(minus_theirs, -1)

    stored = ordered(jnp.concatenate([first_moment, second_moment], axis=1).astype(narrow))
    group = expert_count // 2
    beside = lax.ppermute(stored, "expert", [(e, (e + group) % expert_count) for e in range(expert_count)])
    upper = lax.axis_index("expert") // group
    low = jnp.where(upper == 0, stored, beside)
    high = jnp.where(upper == 0, beside, stored)
    group_pick = lax.dynamic_slice_in_dim(pick, upper * group, group, 0)
    moments_sent = choose(group_pick, jnp.concatenate([low, high], axis=1))
    moments_here = lax.all_to_all(
        moments_sent, "expert", split_axis=0, concat_axis=0, tiled=True,
        axis_index_groups=[list(range(group)), list(range(group, expert_count))],
    )

    turned, far_tok, far_turned = pl.pallas_call(
        turn_kernel,
        in_specs=in_smem() + in_vmem(2),
        out_specs=in_vmem(3),
        out_shape=[
            jax.ShapeDtypeStruct((wide, 2 * row_total), narrow),
            jax.ShapeDtypeStruct((2 * row_total, 2 * own_count), narrow),
            jax.ShapeDtypeStruct((2 * own_count, 2 * row_total), narrow),
        ],
        name="turn",
        compiler_params=pltpu.CompilerParams(vmem_limit_bytes=12 * MEBI),
    )(place, inputs, tok_theirs)
    piece = jax.ShapeDtypeStruct((own_count, part_cols), narrow)
    partial = pl.pallas_call(
        partial_kernel,
        in_specs=in_smem() + in_vmem(8),
        out_specs=in_vmem(1)[0],
        out_shape=jax.ShapeDtypeStruct((2 * row_total, part_cols), jnp.float32),
        scratch_shapes=[pltpu.VMEM((3, 2 * own_count, part_cols), narrow)],
        name="partial",
        compiler_params=pltpu.CompilerParams(vmem_limit_bytes=10 * MEBI),
    )(place, inputs, tok_theirs, mine, theirs, minus_mine, minus_theirs, plus_mine, plus_theirs)
    grad_proj, send_mine, send_theirs = pl.pallas_call(
        project_kernel,
        in_specs=in_smem() + in_vmem(7),
        out_specs=in_vmem(3),
        out_shape=[jax.ShapeDtypeStruct((2 * row_total, part_cols), narrow), piece, piece],
        scratch_shapes=[pltpu.VMEM((2 * own_count, part_cols), narrow)],
        name="project",
        compiler_params=pltpu.CompilerParams(vmem_limit_bytes=8 * MEBI),
    )(place, partial, hid_mine, hid_theirs, far_mine, far_theirs, far_tok, far_turned)
    got_plus = shift(send_mine, 1)
    got_minus = shift(send_theirs, -1)
    next_mine, next_theirs, last_mine, last_theirs, sum_mine, sum_theirs = pl.pallas_call(
        term_kernel,
        in_specs=in_smem() + in_vmem(2),
        out_specs=in_vmem(6),
        out_shape=[piece] * 6,
        name="terms",
        compiler_params=pltpu.CompilerParams(vmem_limit_bytes=8 * MEBI),
    )(place, turned, grad_proj)
    early_theirs = shift(next_theirs, 1)
    early_mine = shift(last_mine, -1)
    late_mine = shift(add(next_mine, got_plus), 1)
    late_theirs = shift(add(last_theirs, got_minus), -1)
    late_mine, late_theirs, moments_here = lax.optimization_barrier((late_mine, late_theirs, moments_here))
    total_other = swap(add(sum_theirs, early_theirs, late_theirs))
    total = jnp.concatenate([add(sum_mine, early_mine, late_mine), total_other], axis=1)
    home = exchange(total.reshape(expert_count, span_rows, col_total))

    def moment_rows(kind):
        sides = [
            moments_here[:, (2 * side + kind) * span_rows : (2 * side + kind + 1) * span_rows]
            for side in range(2)
        ]
        return rows_of(jnp.concatenate(sides, axis=0))

    grad_rows = rows_of(exchange(choose(same, home)))
    bands = chip_count
    band = own_count // bands
    spec = pl.BlockSpec((band, col_total), lambda i: (i, 0))
    out_spec = pl.BlockSpec((1, band, col_total), lambda i: (0, i, 0))
    shape = (1, own_count, col_total)
    return pl.pallas_call(
        adam_kernel,
        grid=(bands,),
        in_specs=in_smem() + [spec] * 4,
        out_specs=[out_spec] * 3,
        out_shape=[
            jax.ShapeDtypeStruct(shape, narrow),
            jax.ShapeDtypeStruct(shape, jnp.float32),
            jax.ShapeDtypeStruct(shape, jnp.float32),
        ],
        name="adam",
        compiler_params=pltpu.CompilerParams(vmem_limit_bytes=12 * MEBI),
    )(
        place, own_rows, moment_rows(0), moment_rows(1), grad_rows,
    )


def solution(mesh):
    in_specs = (
        P(None, ("dp", "expert"), None),
        P(None, ("dp", "expert"), None),
        P(None, ("dp", "expert"), None),
        P(),
        P("dp", "expert"),
        P("dp", "expert", None, None),
        P("dp", "expert", None, None),
    )
    out_specs = (P("expert", "dp", None), P("expert", "dp", None), P("expert", "dp", None))

    return jax.shard_map(on_device, mesh=mesh, in_specs=in_specs, out_specs=out_specs, check_vma=False)
```

```python
import jax
import jax.numpy as jnp
from jax import lax
from jax.experimental import pallas as pl
from jax.experimental.pallas import tpu as pltpu
from jax.sharding import PartitionSpec as P


BLOCK = 128
MEBI = 1 << 20


beta_first = 0.9
beta_second = 0.95
learning_rate = 0.001
weight_decay = 0.1
adam_epsilon = 1e-08
adam_steps = 10.0


def adam_update(params, first_moment, second_moment, gradient):
    moment_one = beta_first * first_moment + (1.0 - beta_first) * gradient
    moment_two = beta_second * second_moment + (1.0 - beta_second) * gradient * gradient
    correct_one = 1.0 - beta_first**adam_steps
    correct_two = 1.0 - beta_second**adam_steps
    params_full = params.astype(jnp.float32)
    step_size = (
        moment_one / correct_one / (jnp.sqrt(moment_two / correct_two) + adam_epsilon)
        + weight_decay * params_full
    )
    return ((params_full - learning_rate * step_size).astype(jnp.bfloat16), moment_one, moment_two)


def grad_halves(projected, upstream):
    half_width = projected.shape[1] // 2
    gate_part = projected[:, :half_width]
    upward = projected[:, half_width:]
    sigmoid_gate = jax.nn.sigmoid(gate_part)
    masked = upstream.astype(jnp.float32)
    grad_gate = masked * upward * sigmoid_gate * (1.0 + gate_part * (1.0 - sigmoid_gate))
    grad_upward = masked * gate_part * sigmoid_gate
    return grad_gate.astype(jnp.bfloat16), grad_upward.astype(jnp.bfloat16)


def term_rows(turned_ref, grad_ref, start, count):
    rows = turned_ref[pl.ds(pl.multiple_of(start, 16), count), :]
    return jnp.dot(rows, grad_ref[...], preferred_element_type=jnp.float32).astype(jnp.bfloat16)


def piece_start(place, step, side, count):
    return pl.multiple_of((2 * ((place[0] + step) % 4) + (place[1] + side) % 2) * count, 16)


def block_start(place, step, count):
    return pl.multiple_of(((place[0] + step) % 4) * 2 * count, 128)


def join(place, block, mine, theirs):
    count = mine.shape[0]
    core = place[1]
    block[pl.ds(pl.multiple_of(core * count, 16), count), :] = mine[...]
    block[pl.ds(pl.multiple_of((1 - core) * count, 16), count), :] = theirs[...]


def partial_kernel(place, tok_mine, tok_theirs, *rest):
    pieces, partial, block = rest[:6], rest[6], rest[7]
    count = pieces[0].shape[0]
    half = tok_mine.shape[0]
    for slot in range(3):
        join(place, block.at[slot], pieces[2 * slot], pieces[2 * slot + 1])
    for low, tok in ((0, tok_mine), (half, tok_theirs)):
        total = None
        for slot, step in enumerate((0, 1, 3)):
            part = jnp.dot(
                tok[:, pl.ds(block_start(place, step, count), 2 * count)],
                block[slot],
                preferred_element_type=jnp.float32,
            )
            total = part if total is None else total + part
        partial[low : low + half, :] = total


def project_kernel(
    place, partial, hid_mine, hid_theirs, piece_mine, piece_theirs, far_tok, far_turned,
    grad_ref, far_mine, far_theirs, block,
):
    count = piece_mine.shape[0]
    half = hid_mine.shape[0]
    width = block.shape[1] // 2
    join(place, block, piece_mine, piece_theirs)
    for hid, low in ((hid_mine, 0), (hid_theirs, half)):
        projected = partial[low : low + half, :] + jnp.dot(
            far_tok[low : low + half, :], block[...], preferred_element_type=jnp.float32
        )
        grad_gate, grad_up = grad_halves(projected, hid[...])
        grad_ref[low : low + half, :width] = grad_gate
        grad_ref[low : low + half, width:] = grad_up
    for out, core in ((far_mine, place[1]), (far_theirs, 1 - place[1])):
        out[...] = term_rows(far_turned, grad_ref, core * count, count)


def turn_kernel(place, tok_mine, tok_theirs, turned, far_tok, far_turned):
    half, wide = tok_mine.shape
    far = far_tok.shape[1]
    begin = pl.multiple_of(((place[0] + 2) % 4) * far, 128)
    for low, tok in ((0, tok_mine), (half, tok_theirs)):
        for step in range(0, wide, 512):
            turned[step : step + 512, low : low + half] = tok[:, step : step + 512].T
        far_tok[low : low + half, :] = tok[:, pl.ds(begin, far)]
    far_turned[...] = turned[pl.ds(begin, far), :]


def term_kernel(place, turned, grad_ref, *outs):
    count = outs[0].shape[0]
    for slot, (step, side) in enumerate(((1, 0), (1, 1), (3, 0), (3, 1), (0, 0), (0, 1))):
        outs[slot][...] = term_rows(turned, grad_ref, piece_start(place, step, side, count), count)


def adam_kernel(place, params, first, second, gradient, updated, moment_one, moment_two):
    lanes = params.shape[1] // 4
    for kind in range(2):
        for side in range(2):
            read = pl.ds((2 * side + kind) * lanes, lanes)
            into = pl.ds(pl.multiple_of((2 * kind + (place[1] + side) % 2) * lanes, 128), lanes)
            new_params, new_one, new_two = adam_update(
                params[:, read],
                first[:, read].astype(jnp.float32),
                second[:, read].astype(jnp.float32),
                gradient[:, read].astype(jnp.float32),
            )
            updated[0, :, into] = new_params
            moment_one[0, :, into] = new_one
            moment_two[0, :, into] = new_two


def in_vmem(count):
    return [pl.BlockSpec(memory_space=pltpu.VMEM) for _ in range(count)]


def in_smem():
    return [pl.BlockSpec(memory_space=pltpu.SMEM)]


def on_device(weights, first_moment, second_moment, placement, block_counts, tokens, hidden_grad):
    expert_count = lax.axis_size("expert")
    dp_count = lax.axis_size("dp")
    chip_count = dp_count // 2
    block_total = weights.shape[0]
    span_rows = weights.shape[1]
    col_total = weights.shape[2]
    inputs = tokens[0, 0]
    row_total, wide = inputs.shape
    narrow = jnp.bfloat16
    own_count = expert_count * span_rows
    quarter = col_total // 4
    part_cols = 2 * quarter
    position = lax.axis_index("dp")
    chip, core = position // 2, position % 2
    place = jnp.stack([chip, core]).astype(jnp.int32)
    pick = (placement[:, None] == jnp.arange(block_total)[None, :]).astype(narrow)
    same = (placement[:, None] == placement[None, :]).astype(narrow)

    def exchange(values):
        return lax.all_to_all(values, "expert", split_axis=0, concat_axis=0, tiled=True)

    def choose(table, values):
        return jnp.einsum("jk,krc->jrc", table, values, preferred_element_type=jnp.float32).astype(narrow)

    def shift(value, step, cross=0):
        pairs = [
            (2 * h + c, 2 * ((h + step) % chip_count) + (c ^ cross))
            for h in range(chip_count)
            for c in range(2)
        ]
        return lax.ppermute(value, "dp", pairs)

    def swap(value):
        return lax.ppermute(value, "dp", [(i, i ^ 1) for i in range(dp_count)])

    def halves(value):
        starts = range(0, value.shape[-1], 2 * quarter)
        even = jnp.concatenate([value[..., k : k + quarter] for k in starts], axis=-1)
        odd = jnp.concatenate([value[..., k + quarter : k + 2 * quarter] for k in starts], axis=-1)
        return jnp.where(core == 0, even, odd), jnp.where(core == 0, odd, even)

    def ordered(value):
        return jnp.concatenate(halves(value), axis=-1)

    def rows_of(value):
        return lax.optimization_barrier(value.reshape(own_count, value.shape[-1]))

    def add(*values):
        total = values[0].astype(jnp.float32)
        for value in values[1:]:
            total = total + value.astype(jnp.float32)
        return total.astype(narrow)

    live_mask = (jnp.arange(row_total) < BLOCK * block_counts[0, 0])[:, None]
    masked = jnp.where(live_mask, hidden_grad[0, 0], jnp.zeros((), narrow))
    hid_mine, hid_give = halves(masked)
    arrived = exchange(choose(pick, ordered(weights)))
    own_rows = arrived.reshape(own_count, col_total)
    mine, give = own_rows[:, :part_cols], own_rows[:, part_cols:]
    tok_theirs = swap(inputs)
    hid_theirs = swap(hid_give)
    plus_mine = shift(mine, 1)
    minus_mine = shift(mine, -1)
    theirs = swap(give)
    minus_theirs = shift(give, -1, 1)
    plus_theirs = shift(give, 1, 1)
    far_mine = shift(plus_mine, 1)
    far_theirs = shift(minus_theirs, -1)

    stored = ordered(jnp.concatenate([first_moment, second_moment], axis=1).astype(narrow))
    group = expert_count // 2
    beside = lax.ppermute(stored, "expert", [(e, (e + group) % expert_count) for e in range(expert_count)])
    upper = lax.axis_index("expert") // group
    low = jnp.where(upper == 0, stored, beside)
    high = jnp.where(upper == 0, beside, stored)
    group_pick = lax.dynamic_slice_in_dim(pick, upper * group, group, 0)
    moments_sent = choose(group_pick, jnp.concatenate([low, high], axis=1))
    moments_here = lax.all_to_all(
        moments_sent, "expert", split_axis=0, concat_axis=0, tiled=True,
        axis_index_groups=[list(range(group)), list(range(group, expert_count))],
    )

    turned, far_tok, far_turned = pl.pallas_call(
        turn_kernel,
        in_specs=in_smem() + in_vmem(2),
        out_specs=in_vmem(3),
        out_shape=[
            jax.ShapeDtypeStruct((wide, 2 * row_total), narrow),
            jax.ShapeDtypeStruct((2 * row_total, 2 * own_count), narrow),
            jax.ShapeDtypeStruct((2 * own_count, 2 * row_total), narrow),
        ],
        name="turn",
        compiler_params=pltpu.CompilerParams(vmem_limit_bytes=12 * MEBI),
    )(place, inputs, tok_theirs)
    piece = jax.ShapeDtypeStruct((own_count, part_cols), narrow)
    partial = pl.pallas_call(
        partial_kernel,
        in_specs=in_smem() + in_vmem(8),
        out_specs=in_vmem(1)[0],
        out_shape=jax.ShapeDtypeStruct((2 * row_total, part_cols), jnp.float32),
        scratch_shapes=[pltpu.VMEM((3, 2 * own_count, part_cols), narrow)],
        name="partial",
        compiler_params=pltpu.CompilerParams(vmem_limit_bytes=10 * MEBI),
    )(place, inputs, tok_theirs, mine, theirs, minus_mine, minus_theirs, plus_mine, plus_theirs)
    grad_proj, send_mine, send_theirs = pl.pallas_call(
        project_kernel,
        in_specs=in_smem() + in_vmem(7),
        out_specs=in_vmem(3),
        out_shape=[jax.ShapeDtypeStruct((2 * row_total, part_cols), narrow), piece, piece],
        scratch_shapes=[pltpu.VMEM((2 * own_count, part_cols), narrow)],
        name="project",
        compiler_params=pltpu.CompilerParams(vmem_limit_bytes=8 * MEBI),
    )(place, partial, hid_mine, hid_theirs, far_mine, far_theirs, far_tok, far_turned)
    got_plus = shift(send_mine, 1)
    got_minus = shift(send_theirs, -1)
    next_mine, next_theirs, last_mine, last_theirs, sum_mine, sum_theirs = pl.pallas_call(
        term_kernel,
        in_specs=in_smem() + in_vmem(2),
        out_specs=in_vmem(6),
        out_shape=[piece] * 6,
        name="terms",
        compiler_params=pltpu.CompilerParams(vmem_limit_bytes=8 * MEBI),
    )(place, turned, grad_proj)
    early_other = shift(next_theirs, 1, 1)
    early_mine = shift(last_mine, -1)
    base_other = swap(sum_theirs)
    late_mine = shift(add(next_mine, got_plus), 1)
    late_other = shift(add(last_theirs, got_minus), -1, 1)
    late_mine, late_other, moments_here = lax.optimization_barrier((late_mine, late_other, moments_here))
    total = jnp.concatenate(
        [add(sum_mine, early_mine, late_mine), add(base_other, early_other, late_other)], axis=1
    )
    home = exchange(total.reshape(expert_count, span_rows, col_total))

    def moment_rows(kind):
        sides = [
            moments_here[:, (2 * side + kind) * span_rows : (2 * side + kind + 1) * span_rows]
            for side in range(2)
        ]
        return rows_of(jnp.concatenate(sides, axis=0))

    grad_rows = rows_of(exchange(choose(same, home)))
    bands = span_rows
    band = own_count // bands
    spec = pl.BlockSpec((band, col_total), lambda i: (i, 0))
    out_spec = pl.BlockSpec((1, band, col_total), lambda i: (0, i, 0))
    shape = (1, own_count, col_total)
    return pl.pallas_call(
        adam_kernel,
        grid=(bands,),
        in_specs=in_smem() + [spec] * 4,
        out_specs=[out_spec] * 3,
        out_shape=[
            jax.ShapeDtypeStruct(shape, narrow),
            jax.ShapeDtypeStruct(shape, jnp.float32),
            jax.ShapeDtypeStruct(shape, jnp.float32),
        ],
        name="adam",
        compiler_params=pltpu.CompilerParams(vmem_limit_bytes=12 * MEBI),
    )(
        place, own_rows, moment_rows(0), moment_rows(1), grad_rows,
    )


def solution(mesh):
    in_specs = (
        P(None, ("dp", "expert"), None),
        P(None, ("dp", "expert"), None),
        P(None, ("dp", "expert"), None),
        P(),
        P("dp", "expert"),
        P("dp", "expert", None, None),
        P("dp", "expert", None, None),
    )
    out_specs = (P("expert", "dp", None), P("expert", "dp", None), P("expert", "dp", None))

    return jax.shard_map(on_device, mesh=mesh, in_specs=in_specs, out_specs=out_specs, check_vma=False)
```

```python
import jax
import jax.numpy as jnp
from jax import lax
from jax.experimental import pallas as pl
from jax.experimental.pallas import tpu as pltpu
from jax.sharding import PartitionSpec as P


BLOCK = 128
MEBI = 1 << 20


beta_first = 0.9
beta_second = 0.95
learning_rate = 0.001
weight_decay = 0.1
adam_epsilon = 1e-08
adam_steps = 10.0


def adam_update(params, first_moment, second_moment, gradient):
    moment_one = beta_first * first_moment + (1.0 - beta_first) * gradient
    moment_two = beta_second * second_moment + (1.0 - beta_second) * gradient * gradient
    correct_one = 1.0 - beta_first**adam_steps
    correct_two = 1.0 - beta_second**adam_steps
    params_full = params.astype(jnp.float32)
    step_size = (
        moment_one / correct_one / (jnp.sqrt(moment_two / correct_two) + adam_epsilon)
        + weight_decay * params_full
    )
    return ((params_full - learning_rate * step_size).astype(jnp.bfloat16), moment_one, moment_two)


def grad_halves(projected, upstream):
    half_width = projected.shape[1] // 2
    gate_part = projected[:, :half_width]
    upward = projected[:, half_width:]
    sigmoid_gate = jax.nn.sigmoid(gate_part)
    masked = upstream.astype(jnp.float32)
    grad_gate = masked * upward * sigmoid_gate * (1.0 + gate_part * (1.0 - sigmoid_gate))
    grad_upward = masked * gate_part * sigmoid_gate
    return grad_gate.astype(jnp.bfloat16), grad_upward.astype(jnp.bfloat16)


def term_rows(turned_ref, grad_ref, start, count):
    rows = turned_ref[pl.ds(pl.multiple_of(start, 16), count), :]
    return jnp.dot(rows, grad_ref[...], preferred_element_type=jnp.float32).astype(jnp.bfloat16)


def chip_at(place, step):
    return (place[0] + step * (1 + 2 * place[1])) % 4


def piece_start(place, step, side, count):
    return pl.multiple_of((2 * chip_at(place, step) + (place[1] + side) % 2) * count, 16)


def block_start(place, step, count):
    return pl.multiple_of(chip_at(place, step) * 2 * count, 128)


def join(place, block, mine, theirs):
    count = mine.shape[0]
    core = place[1]
    block[pl.ds(pl.multiple_of(core * count, 16), count), :] = mine[...]
    block[pl.ds(pl.multiple_of((1 - core) * count, 16), count), :] = theirs[...]


def partial_kernel(place, tok_mine, tok_theirs, *rest):
    pieces, partial, block = rest[:6], rest[6], rest[7]
    count = pieces[0].shape[0]
    half = tok_mine.shape[0]
    for slot in range(3):
        join(place, block.at[slot], pieces[2 * slot], pieces[2 * slot + 1])
    for low, tok in ((0, tok_mine), (half, tok_theirs)):
        total = None
        for slot, step in enumerate((0, 1, 3)):
            part = jnp.dot(
                tok[:, pl.ds(block_start(place, step, count), 2 * count)],
                block[slot],
                preferred_element_type=jnp.float32,
            )
            total = part if total is None else total + part
        partial[low : low + half, :] = total


def project_kernel(
    place, partial, hid_mine, hid_theirs, piece_mine, piece_theirs, far_tok, far_turned,
    grad_ref, far_mine, far_theirs, block,
):
    count = piece_mine.shape[0]
    half = hid_mine.shape[0]
    width = block.shape[1] // 2
    join(place, block, piece_mine, piece_theirs)
    for hid, low in ((hid_mine, 0), (hid_theirs, half)):
        projected = partial[low : low + half, :] + jnp.dot(
            far_tok[low : low + half, :], block[...], preferred_element_type=jnp.float32
        )
        grad_gate, grad_up = grad_halves(projected, hid[...])
        grad_ref[low : low + half, :width] = grad_gate
        grad_ref[low : low + half, width:] = grad_up
    for out, core in ((far_mine, place[1]), (far_theirs, 1 - place[1])):
        out[...] = term_rows(far_turned, grad_ref, core * count, count)


def turn_kernel(place, tok_mine, tok_theirs, turned, far_tok, far_turned):
    half, wide = tok_mine.shape
    far = far_tok.shape[1]
    begin = pl.multiple_of(((place[0] + 2) % 4) * far, 128)
    for low, tok in ((0, tok_mine), (half, tok_theirs)):
        for step in range(0, wide, 512):
            turned[step : step + 512, low : low + half] = tok[:, step : step + 512].T
        far_tok[low : low + half, :] = tok[:, pl.ds(begin, far)]
    far_turned[...] = turned[pl.ds(begin, far), :]


def term_kernel(place, turned, grad_ref, *outs):
    count = outs[0].shape[0]
    for slot, (step, side) in enumerate(((1, 0), (1, 1), (3, 0), (3, 1), (0, 0), (0, 1))):
        outs[slot][...] = term_rows(turned, grad_ref, piece_start(place, step, side, count), count)


def adam_kernel(place, params, first, second, gradient, updated, moment_one, moment_two):
    lanes = params.shape[1] // 4
    for kind in range(2):
        for side in range(2):
            read = pl.ds((2 * side + kind) * lanes, lanes)
            into = pl.ds(pl.multiple_of((2 * kind + (place[1] + side) % 2) * lanes, 128), lanes)
            new_params, new_one, new_two = adam_update(
                params[:, read],
                first[:, read].astype(jnp.float32),
                second[:, read].astype(jnp.float32),
                gradient[:, read].astype(jnp.float32),
            )
            updated[0, :, into] = new_params
            moment_one[0, :, into] = new_one
            moment_two[0, :, into] = new_two


def in_vmem(count):
    return [pl.BlockSpec(memory_space=pltpu.VMEM) for _ in range(count)]


def in_smem():
    return [pl.BlockSpec(memory_space=pltpu.SMEM)]


def on_device(weights, first_moment, second_moment, placement, block_counts, tokens, hidden_grad):
    expert_count = lax.axis_size("expert")
    dp_count = lax.axis_size("dp")
    chip_count = dp_count // 2
    block_total = weights.shape[0]
    span_rows = weights.shape[1]
    col_total = weights.shape[2]
    inputs = tokens[0, 0]
    row_total, wide = inputs.shape
    narrow = jnp.bfloat16
    own_count = expert_count * span_rows
    quarter = col_total // 4
    part_cols = 2 * quarter
    position = lax.axis_index("dp")
    chip, core = position // 2, position % 2
    place = jnp.stack([chip, core]).astype(jnp.int32)
    pick = (placement[:, None] == jnp.arange(block_total)[None, :]).astype(narrow)
    same = (placement[:, None] == placement[None, :]).astype(narrow)

    def exchange(values):
        return lax.all_to_all(values, "expert", split_axis=0, concat_axis=0, tiled=True)

    def choose(table, values):
        return jnp.einsum("jk,krc->jrc", table, values, preferred_element_type=jnp.float32).astype(narrow)

    def shift(value, step):
        pairs = [
            (2 * h + c, 2 * ((h + (1 - 2 * c) * step) % chip_count) + c)
            for h in range(chip_count)
            for c in range(2)
        ]
        return lax.ppermute(value, "dp", pairs)

    def shift_other(value, step, sense):
        pairs = [
            (2 * h + c, 2 * ((h + sense * (1 - 2 * c) * step) % chip_count) + 1 - c)
            for h in range(chip_count)
            for c in range(2)
        ]
        return lax.ppermute(value, "dp", pairs)

    def swap(value):
        return lax.ppermute(value, "dp", [(i, i ^ 1) for i in range(dp_count)])

    def halves(value):
        starts = range(0, value.shape[-1], 2 * quarter)
        even = jnp.concatenate([value[..., k : k + quarter] for k in starts], axis=-1)
        odd = jnp.concatenate([value[..., k + quarter : k + 2 * quarter] for k in starts], axis=-1)
        return jnp.where(core == 0, even, odd), jnp.where(core == 0, odd, even)

    def ordered(value):
        return jnp.concatenate(halves(value), axis=-1)

    def rows_of(value):
        return lax.optimization_barrier(value.reshape(own_count, value.shape[-1]))

    def add(*values):
        total = values[0].astype(jnp.float32)
        for value in values[1:]:
            total = total + value.astype(jnp.float32)
        return total.astype(narrow)

    live_mask = (jnp.arange(row_total) < BLOCK * block_counts[0, 0])[:, None]
    masked = jnp.where(live_mask, hidden_grad[0, 0], jnp.zeros((), narrow))
    hid_mine, hid_give = halves(masked)
    arrived = exchange(choose(pick, ordered(weights)))
    own_rows = arrived.reshape(own_count, col_total)
    mine, give = own_rows[:, :part_cols], own_rows[:, part_cols:]
    tok_theirs = swap(inputs)
    hid_theirs = swap(hid_give)
    plus_mine = shift(mine, 1)
    minus_mine = shift(mine, -1)
    theirs = swap(give)
    minus_theirs = shift_other(give, -1, -1)
    plus_theirs = shift_other(give, 1, -1)
    far_mine = shift(plus_mine, 1)
    far_theirs = shift(minus_theirs, -1)

    stored = ordered(jnp.concatenate([first_moment, second_moment], axis=1).astype(narrow))
    group = expert_count // 2
    beside = lax.ppermute(stored, "expert", [(e, (e + group) % expert_count) for e in range(expert_count)])
    upper = lax.axis_index("expert") // group
    low = jnp.where(upper == 0, stored, beside)
    high = jnp.where(upper == 0, beside, stored)
    group_pick = lax.dynamic_slice_in_dim(pick, upper * group, group, 0)
    moments_sent = choose(group_pick, jnp.concatenate([low, high], axis=1))
    moments_here = lax.all_to_all(
        moments_sent, "expert", split_axis=0, concat_axis=0, tiled=True,
        axis_index_groups=[list(range(group)), list(range(group, expert_count))],
    )

    turned, far_tok, far_turned = pl.pallas_call(
        turn_kernel,
        in_specs=in_smem() + in_vmem(2),
        out_specs=in_vmem(3),
        out_shape=[
            jax.ShapeDtypeStruct((wide, 2 * row_total), narrow),
            jax.ShapeDtypeStruct((2 * row_total, 2 * own_count), narrow),
            jax.ShapeDtypeStruct((2 * own_count, 2 * row_total), narrow),
        ],
        name="turn",
        compiler_params=pltpu.CompilerParams(vmem_limit_bytes=12 * MEBI),
    )(place, inputs, tok_theirs)
    piece = jax.ShapeDtypeStruct((own_count, part_cols), narrow)
    partial = pl.pallas_call(
        partial_kernel,
        in_specs=in_smem() + in_vmem(8),
        out_specs=in_vmem(1)[0],
        out_shape=jax.ShapeDtypeStruct((2 * row_total, part_cols), jnp.float32),
        scratch_shapes=[pltpu.VMEM((3, 2 * own_count, part_cols), narrow)],
        name="partial",
        compiler_params=pltpu.CompilerParams(vmem_limit_bytes=10 * MEBI),
    )(place, inputs, tok_theirs, mine, theirs, minus_mine, minus_theirs, plus_mine, plus_theirs)
    grad_proj, send_mine, send_theirs = pl.pallas_call(
        project_kernel,
        in_specs=in_smem() + in_vmem(7),
        out_specs=in_vmem(3),
        out_shape=[jax.ShapeDtypeStruct((2 * row_total, part_cols), narrow), piece, piece],
        scratch_shapes=[pltpu.VMEM((2 * own_count, part_cols), narrow)],
        name="project",
        compiler_params=pltpu.CompilerParams(vmem_limit_bytes=8 * MEBI),
    )(place, partial, hid_mine, hid_theirs, far_mine, far_theirs, far_tok, far_turned)
    got_plus = shift(send_mine, 1)
    got_minus = shift(send_theirs, -1)
    next_mine, next_theirs, last_mine, last_theirs, sum_mine, sum_theirs = pl.pallas_call(
        term_kernel,
        in_specs=in_smem() + in_vmem(2),
        out_specs=in_vmem(6),
        out_shape=[piece] * 6,
        name="terms",
        compiler_params=pltpu.CompilerParams(vmem_limit_bytes=8 * MEBI),
    )(place, turned, grad_proj)
    early_other = shift_other(next_theirs, 1, 1)
    early_mine = shift(last_mine, -1)
    base_other = swap(sum_theirs)
    late_mine = shift(add(next_mine, got_plus), 1)
    late_other = shift_other(add(last_theirs, got_minus), -1, 1)
    late_mine, late_other, moments_here = lax.optimization_barrier((late_mine, late_other, moments_here))
    total = jnp.concatenate(
        [add(sum_mine, early_mine, late_mine), add(base_other, early_other, late_other)], axis=1
    )
    home = exchange(total.reshape(expert_count, span_rows, col_total))

    def moment_rows(kind):
        sides = [
            moments_here[:, (2 * side + kind) * span_rows : (2 * side + kind + 1) * span_rows]
            for side in range(2)
        ]
        return rows_of(jnp.concatenate(sides, axis=0))

    grad_rows = rows_of(exchange(choose(same, home)))
    bands = 2
    band = own_count // bands
    spec = pl.BlockSpec((band, col_total), lambda i: (i, 0))
    out_spec = pl.BlockSpec((1, band, col_total), lambda i: (0, i, 0))
    shape = (1, own_count, col_total)
    return pl.pallas_call(
        adam_kernel,
        grid=(bands,),
        in_specs=in_smem() + [spec] * 4,
        out_specs=[out_spec] * 3,
        out_shape=[
            jax.ShapeDtypeStruct(shape, narrow),
            jax.ShapeDtypeStruct(shape, jnp.float32),
            jax.ShapeDtypeStruct(shape, jnp.float32),
        ],
        name="adam",
        compiler_params=pltpu.CompilerParams(vmem_limit_bytes=12 * MEBI),
    )(
        place, own_rows, moment_rows(0), moment_rows(1), grad_rows,
    )


def solution(mesh):
    in_specs = (
        P(None, ("dp", "expert"), None),
        P(None, ("dp", "expert"), None),
        P(None, ("dp", "expert"), None),
        P(),
        P("dp", "expert"),
        P("dp", "expert", None, None),
        P("dp", "expert", None, None),
    )
    out_specs = (P("expert", "dp", None), P("expert", "dp", None), P("expert", "dp", None))

    return jax.shard_map(on_device, mesh=mesh, in_specs=in_specs, out_specs=out_specs, check_vma=False)
```
